32 devices in a mesh: af: 4 (over y, x), sa: 8 (over z, core).
Axes of the slice: x: 2, y: 2, z: 4, core: 2. Of those that a mesh axis runs over, the one named last changes fastest.
Arguments:
- data_real: bfloat16 [64, 512, 512], P('af', 'sa'), may hold values from -0.5 to 0.5
- data_imaginary: bfloat16 [64, 512, 512], P('af', 'sa'), may hold values from -0.5 to 0.5
- wavelet_real: float32 [64], P('af'), may hold values from -2.5 to 2.5
- wavelet_imaginary: float32 [64], P('af'), may hold values from -2.5 to 2.5
- primaries_real: float32 [64, 512, 512], P('af', 'sa'), may hold values from -3 to 3
- primaries_imaginary: float32 [64, 512, 512], P('af', 'sa'), may hold values from -3 to 3
Outputs:
- updated_real: float32 [64, 512, 512], P('af', 'sa')
- updated_imaginary: float32 [64, 512, 512], P('af', 'sa')
- misfit: float32 [2], replicated
The draws below stay inside these ranges and needn't reach their ends.
All inputs are finite; a program needn't handle non-finite values.
Results may differ from the reference program's by a relative error of at most 0.0018.
Values may be sent and summed in bfloat16 or wider, within the bound.
A program may use at most 128 MiB of HBM per device.

```python
import jax
import jax.numpy as jnp
from jax import lax

N = 512
F = 64
ITERS = 2


def levels(own_key, dims, cuts, low, top_value):
    gain, own = 1.0, jax.random.fold_in(own_key, 6)
    for axis_at, parts in cuts:
        steps = jnp.exp(jax.random.uniform(jax.random.fold_in(own, axis_at), (parts,), jnp.float32, low / len(cuts), top_value / len(cuts)))
        gain = gain * jnp.repeat(steps, dims[axis_at] // parts).reshape([-1 if axis == axis_at else 1 for axis in range(len(dims))])
    return gain


def scatter_about(rng, shape, deviation, most, pieces=(), kind=jnp.bfloat16):
    gain = levels(rng, shape, pieces, -0.22, 0.18) if pieces else 1.0
    result = jax.random.normal(rng, shape, jnp.float32) * deviation * gain
    return jnp.minimum(jnp.maximum(result, -most), most).astype(kind)


def setup_inputs(seed: int = 0) -> dict:
    streams_of = jax.random.split(jax.random.key(seed), 7)
    data_real = scatter_about(streams_of[0], (F, N, N), (N // 4) ** -0.5, 0.5, ((0, 4), (1, 8)))
    data_imaginary = scatter_about(streams_of[1], (F, N, N), (N // 4) ** -0.5, 0.5, ((0, 4), (1, 8)))
    wavelet_real = scatter_about(streams_of[2], (F,), 0.7, 2.5, ((0, 4),), jnp.float32)
    wavelet_imaginary = scatter_about(streams_of[3], (F,), 0.7, 2.5, ((0, 4),), jnp.float32)
    primaries_real = scatter_about(streams_of[4], (F, N, N), 0.5, 3.0, ((0, 4), (1, 8)), jnp.float32)
    primaries_imaginary = scatter_about(streams_of[5], (F, N, N), 0.5, 3.0, ((0, 4), (1, 8)), jnp.float32)
    return dict(data_real=data_real, data_imaginary=data_imaginary, wavelet_real=wavelet_real, wavelet_imaginary=wavelet_imaginary, primaries_real=primaries_real, primaries_imaginary=primaries_imaginary)


STEP_LENGTH = 0.02
THRESHOLD = 0.25


def forward_product(left, right):
    return jnp.einsum("frk,fkc->frc", left, right, precision=lax.Precision.HIGHEST)


def adjoint_product(left, right):
    return jnp.einsum("frk,fjk->frj", left, right, precision=lax.Precision.HIGHEST)


def rounded(values):
    return lax.optimization_barrier(values.astype(jnp.bfloat16)).astype(jnp.float32)


def reference(data_real, data_imaginary, wavelet_real, wavelet_imaginary, primaries_real, primaries_imaginary):
    slab_real = data_real.astype(jnp.float32)
    slab_imaginary = data_imaginary.astype(jnp.float32)
    wave_real = wavelet_real[:, None, None]
    wave_imaginary = wavelet_imaginary[:, None, None]
    current_real = primaries_real
    current_imaginary = primaries_imaginary
    misfits = []
    for iteration in range(ITERS):
        rounded_real = rounded(current_real)
        rounded_imaginary = rounded(current_imaginary)
        forward_real = forward_product(rounded_real, slab_real) - forward_product(rounded_imaginary, slab_imaginary)
        forward_imaginary = forward_product(rounded_real, slab_imaginary) + forward_product(rounded_imaginary, slab_real)
        error_real = slab_real + forward_real - (wave_real * current_real - wave_imaginary * current_imaginary)
        error_imaginary = slab_imaginary + forward_imaginary - (wave_real * current_imaginary + wave_imaginary * current_real)
        total = jnp.sum(error_real * error_real) + jnp.sum(error_imaginary * error_imaginary)
        misfits.append(total / (F * N * N))
        eb_real = rounded(error_real)
        eb_imaginary = rounded(error_imaginary)
        back_real = adjoint_product(eb_real, slab_real) + adjoint_product(eb_imaginary, slab_imaginary)
        back_imaginary = adjoint_product(eb_imaginary, slab_real) - adjoint_product(eb_real, slab_imaginary)
        gradient_real = wave_real * error_real + wave_imaginary * error_imaginary - back_real
        gradient_imaginary = wave_real * error_imaginary - wave_imaginary * error_real - back_imaginary
        stepped_real = current_real + STEP_LENGTH * gradient_real
        stepped_imaginary = current_imaginary + STEP_LENGTH * gradient_imaginary
        in_time = jnp.fft.ifft(stepped_real + 1j * stepped_imaginary, axis=0, norm="ortho")
        time_real = jnp.real(in_time)
        time_imaginary = jnp.imag(in_time)
        shrunk_real = time_real - jnp.clip(time_real, -THRESHOLD, THRESHOLD)
        shrunk_imaginary = time_imaginary - jnp.clip(time_imaginary, -THRESHOLD, THRESHOLD)
        in_frequency = jnp.fft.fft(shrunk_real + 1j * shrunk_imaginary, axis=0, norm="ortho")
        current_real = jnp.real(in_frequency).astype(jnp.float32)
        current_imaginary = jnp.imag(in_frequency).astype(jnp.float32)
    return current_real, current_imaginary, jnp.stack(misfits).astype(jnp.float32)
```

```python
import functools
import math

import jax
import jax.numpy as jnp
import numpy as np
from jax import lax
from jax.experimental import pallas as pl
from jax.experimental.pallas import tpu as pltpu
from jax.sharding import PartitionSpec as P

ITERS = 2
STEP_LENGTH = 0.02
THRESHOLD = 0.25
RADIX = 8
HALF = math.sqrt(0.5)
REACH = 64.0
TINY = 2.0**-126
MESH = pl.DeviceIdType.MESH


def encode(x):
    y = x * (1.0 / REACH)
    return ((y * y) * (y * jnp.abs(y))).astype(jnp.bfloat16)


def decode(code):
    v = code.astype(jnp.float32)
    r = lax.rsqrt(lax.rsqrt(jnp.maximum(jnp.abs(v), TINY))) * REACH
    return jnp.where(v > 0, r, jnp.where(v < 0, -r, 0.0))


def add(a, b):
    return (a[0] + b[0], a[1] + b[1])


def sub(a, b):
    return (a[0] - b[0], a[1] - b[1])


def turn(a, sign):
    return (-a[1], a[0]) if sign > 0 else (a[1], -a[0])


def rotate(a, c, s):
    return (a[0] * c - a[1] * s, a[0] * s + a[1] * c)


def four(a, b, c, d, sign):
    s0, s1, s2, s3 = add(a, c), sub(a, c), add(b, d), turn(sub(b, d), sign)
    return add(s0, s2), add(s1, s3), sub(s0, s2), sub(s1, s3)


def eight(x, sign):
    even = four(x[0], x[2], x[4], x[6], sign)
    odd = four(x[1], x[3], x[5], x[7], sign)
    o1 = add(odd[1], turn(odd[1], sign))
    o3 = sub(turn(odd[3], sign), odd[3])
    odd = (odd[0], (o1[0] * HALF, o1[1] * HALF), turn(odd[2], sign), (o3[0] * HALF, o3[1] * HALF))
    return [add(even[k], odd[k]) for k in range(4)] + [sub(even[k], odd[k]) for k in range(4)]


def shrink(v):
    return v - jnp.clip(v, -THRESHOLD, THRESHOLD)


def loop(start, stop, body):
    def step(i, _):
        body(i)
        return 0

    lax.fori_loop(start, stop, step, 0)


def kernel(
    A, S, chunks, wr, wi, twiddle, data_r, data_i, prim_r, prim_i, out, mis,
    whole, current, initial, work, traces, hs, hr, gs, gr, squares, by_af, by_sa,
    local_sem, up_sem, down_sem, ring_sem, pair_send, pair_recv,
    init_send, init_recv, h_send, h_recv, g_send, g_recv, m_send, m_recv,
):
    C = S // 2
    U, _, R, N = data_r.shape
    W = N // A
    per = RADIX // chunks
    rows = 16 if R % 16 == 0 else 8
    a = lax.axis_index("af")
    s = lax.axis_index("sa")
    c = s // 2
    k = s % 2
    partner = c * 2 + 1 - k
    mine = pl.ds(pl.multiple_of(a * W, W), W)

    def cols(b):
        return pl.ds(pl.multiple_of(b * W, W), W)

    def ahead(j):
        return lax.rem(a + j, A)

    def behind(j):
        return lax.rem(a + A - j, A)

    barrier = pltpu.get_barrier_semaphore()
    for j in range(1, A):
        pl.semaphore_signal(barrier, inc=1, device_id=(ahead(j), s), device_id_type=MESH)
    loop(
        1, S,
        lambda j: pl.semaphore_signal(barrier, inc=1, device_id=(a, lax.rem(s + j, S)), device_id_type=MESH),
    )

    locals_ = [
        pltpu.make_async_copy(data_r, whole.at[:, :, 0, s], local_sem.at[0]),
        pltpu.make_async_copy(data_i, whole.at[:, :, 1, s], local_sem.at[1]),
        pltpu.make_async_copy(prim_r, current.at[0], local_sem.at[2]),
        pltpu.make_async_copy(prim_i, current.at[1], local_sem.at[3]),
        pltpu.make_async_copy(prim_r.at[:, :, :, mine], initial.at[0, a], local_sem.at[4]),
        pltpu.make_async_copy(prim_i.at[:, :, :, mine], initial.at[1, a], local_sem.at[5]),
    ]
    for copy in locals_:
        copy.start()
    squares[...] = jnp.zeros_like(squares)
    pl.semaphore_wait(barrier, A - 1 + S - 1)

    def shard(chip, core, h):
        return whole.at[:, pl.ds(h * per, per), :, chip * 2 + core]

    def remote(src, dst, send, recv, device):
        return pltpu.make_async_remote_copy(
            src_ref=src, dst_ref=dst, send_sem=send, recv_sem=recv, device_id=device, device_id_type=MESH
        )

    def up(chip, h):
        ref = shard(chip, k, h)
        return remote(ref, ref, up_sem.at[chip, h], ring_sem.at[chip, h], (a, lax.rem(s + 2, S)))

    def down(chip, h):
        ref = shard(chip, k, h)
        return remote(ref, ref, down_sem.at[chip, h], ring_sem.at[chip, h], (a, lax.rem(s + S - 2, S)))

    def across(chip, h):
        ref = shard(chip, k, h)
        return remote(ref, ref, pair_send.at[chip, h], pair_recv.at[chip, h], (a, partner))

    def across_in(chip, h):
        ref = shard(chip, 1 - k, h)
        return remote(ref, ref, pair_send.at[chip, h], pair_recv.at[chip, h], (a, partner))

    def initials(part, j):
        src = (prim_r, prim_i)[part]
        return remote(
            src.at[:, :, :, cols(ahead(j))], initial.at[part, a],
            init_send.at[part, j], init_recv.at[part, j], (ahead(j), s),
        )

    def initials_in(part, j):
        src = (prim_r, prim_i)[part]
        return remote(
            src.at[:, :, :, mine], initial.at[part, behind(j)],
            init_send.at[part, j], init_recv.at[part, j], (ahead(j), s),
        )

    locals_[0].wait()
    locals_[1].wait()

    def first(h):
        @pl.when(c + 1 < C)
        def _():
            up(c, h).start()

        @pl.when(c > 0)
        def _():
            down(c, h).start()

        across(c, h).start()

    loop(0, chunks, first)
    for j in range(1, A):
        for part in range(2):
            initials(part, j).start()

    def arrive(d, h):
        @pl.when(c >= d)
        def _():
            src = c - d
            up(src, h).wait_recv()
            across(src, h).start()

            @pl.when(c + 1 < C)
            def _():
                up(src, h).start()

        @pl.when(c + d < C)
        def _():
            src = c + d
            down(src, h).wait_recv()
            across(src, h).start()

            @pl.when(c > 0)
            def _():
                down(src, h).start()

    loop(1, C - 1, lambda d: loop(0, chunks, lambda h: arrive(d, h)))

    def h_copy(j, f):
        to = ahead(j)
        return remote(
            hs.at[to, :, :, f], hr.at[a, :, :, f], h_send.at[j, f], h_recv.at[j, f], (to, s)
        )

    def h_copy_in(j, f):
        return remote(
            hs.at[a, :, :, f], hr.at[behind(j), :, :, f], h_send.at[j, f], h_recv.at[j, f], (ahead(j), s)
        )

    def g_copy(it, j, f):
        to = ahead(j)
        dst = gr if it == 0 else out
        return remote(
            gs.at[to, :, :, f], dst.at[:, :, f, :, mine],
            g_send.at[it, j, f], g_recv.at[it, j, f], (to, s),
        )

    def g_copy_in(it, j, f):
        dst = gr if it == 0 else out
        return remote(
            gs.at[a, :, :, f], dst.at[:, :, f, :, cols(behind(j))],
            g_send.at[it, j, f], g_recv.at[it, j, f], (ahead(j), s),
        )

    def product(it, f):
        def one(u):
            qr = wr[u * RADIX + f]
            qi = wi[u * RADIX + f]
            if it == 0:
                re = current[0, u, f]
                im = current[1, u, f]
            else:
                re = gr[0, u, f].astype(jnp.float32)
                im = gr[1, u, f].astype(jnp.float32)
            whole_r = whole[u, f, 0].reshape(N, N)
            whole_i = whole[u, f, 1].reshape(N, N)
            left = jnp.concatenate([re.astype(jnp.bfloat16), im.astype(jnp.bfloat16)], axis=0)
            pr = jnp.dot(left, whole_r, preferred_element_type=jnp.float32)
            pi = jnp.dot(left, whole_i, preferred_element_type=jnp.float32)
            er = whole[u, f, 0, s].astype(jnp.float32) + (pr[:R] - pi[R:]) - (qr * re - qi * im)
            ei = whole[u, f, 1, s].astype(jnp.float32) + (pi[:R] + pr[R:]) - (qr * im + qi * re)
            sq = er * er + ei * ei
            part = sq[:8]
            for i in range(1, R // 8):
                part = part + sq[i * 8 : (i + 1) * 8]
            row = part[:, :128]
            for i in range(1, N // 128):
                row = row + part[:, i * 128 : (i + 1) * 128]
            squares[it] += row
            eb = jnp.concatenate([er.astype(jnp.bfloat16), ei.astype(jnp.bfloat16)], axis=0)
            dims = (((1,), (1,)), ((), ()))
            br = lax.dot_general(eb, whole_r, dims, preferred_element_type=jnp.float32)
            bi = lax.dot_general(eb, whole_i, dims, preferred_element_type=jnp.float32)
            dr = encode(STEP_LENGTH * (qr * er + qi * ei - (br[:R] + bi[R:])))
            di = encode(STEP_LENGTH * (qr * ei - qi * er - (br[R:] - bi[:R])))
            for b in range(A):
                hs[b, 0, u, f] = dr[:, b * W : (b + 1) * W]
                hs[b, 1, u, f] = di[:, b * W : (b + 1) * W]
            hr[a, 0, u, f] = hs[a, 0, u, f]
            hr[a, 1, u, f] = hs[a, 1, u, f]

        loop(0, U, one)
        for j in range(1, A):
            h_copy(j, f).start()

    def stage_in(it, f):
        for j in range(1, A):
            h_copy_in(j, f).wait_recv()

        def some(g):
            at = pl.ds(pl.multiple_of(g * rows, rows), rows)
            x = []
            for f2 in range(RADIX):
                b, u = divmod(f2, U)
                re = decode(hr[b, 0, u, f, at, :])
                im = decode(hr[b, 1, u, f, at, :])
                if it == 0:
                    re = re + initial[0, b, u, f, at, :]
                    im = im + initial[1, b, u, f, at, :]
                x.append((re * (1.0 / RADIX), im * (1.0 / RADIX)))
            y = eight(x, 1)
            for t in range(RADIX):
                v = rotate(y[t], twiddle[0, f * t], twiddle[1, f * t]) if t else y[t]
                work[0, f, t, at, :] = v[0]
                work[1, f, t, at, :] = v[1]

        loop(0, R // rows, some)

    def stage_time(it):
        def some(g):
            at = pl.ds(pl.multiple_of(g * rows, rows), rows)

            def one(t):
                y = eight([(work[0, f, t, at, :], work[1, f, t, at, :]) for f in range(RADIX)], 1)
                if it > 0:
                    y = [(v[0] + traces[0, n, t, at, :], v[1] + traces[1, n, t, at, :]) for n, v in enumerate(y)]
                y = [(shrink(v[0]), shrink(v[1])) for v in y]
                if it < ITERS - 1:
                    for n, v in enumerate(y):
                        traces[0, n, t, at, :] = v[0]
                        traces[1, n, t, at, :] = v[1]
                y = eight(y, -1)
                for f in range(RADIX):
                    v = rotate(y[f], twiddle[0, f * t], -twiddle[1, f * t]) if f else y[f]
                    work[0, f, t, at, :] = v[0]
                    work[1, f, t, at, :] = v[1]

            loop(0, RADIX, one)

        loop(0, R // rows, some)

    def stage_out(it, f):
        dst = gr if it == 0 else out

        def some(g):
            at = pl.ds(pl.multiple_of(g * rows, rows), rows)
            y = eight([(work[0, f, t, at, :], work[1, f, t, at, :]) for t in range(RADIX)], -1)
            for f2 in range(RADIX):
                b, u = divmod(f2, U)
                for part in range(2):
                    v = y[f2][part] * (1.0 / RADIX)
                    gs[b, part, u, f, at, :] = v.astype(jnp.bfloat16) if it == 0 else encode(v)

        loop(0, R // rows, some)
        for j in range(1, A):
            g_copy(it, j, f).start()
        for part in range(2):
            for u in range(U):
                dst[part, u, f, :, mine] = gs[a, part, u, f]

    for copy in locals_[2:]:
        copy.wait()
    for j in range(1, A):
        for part in range(2):
            initials_in(part, j).wait_recv()

    def last(h):
        arrive(C - 1, h)
        loop(0, C, lambda chip: across_in(chip, h).wait_recv())
        loop(0, per, lambda i: product(0, h * per + i))

        @pl.when(h > 0)
        def _():
            loop(0, per, lambda i: stage_in(0, (h - 1) * per + i))

    loop(0, chunks, last)
    loop(0, per, lambda i: stage_in(0, (chunks - 1) * per + i))
    stage_time(0)
    loop(0, RADIX, lambda f: stage_out(0, f))

    def h_sent(f):
        for j in range(1, A):
            h_copy(j, f).wait_send()

    loop(0, RADIX, h_sent)

    def again(f):
        for j in range(1, A):
            g_copy_in(0, j, f).wait_recv()
        product(1, f)

        @pl.when(f > 0)
        def _():
            stage_in(1, f - 1)

    loop(0, RADIX, again)
    by_af[a] = squares[...]

    def af_copy(j):
        return remote(squares, by_af.at[a], m_send.at[j], m_recv.at[j], (ahead(j), s))

    def af_copy_in(j):
        return remote(squares, by_af.at[behind(j)], m_send.at[j], m_recv.at[j], (ahead(j), s))

    for j in range(1, A):
        af_copy(j).start()
    stage_in(1, RADIX - 1)
    stage_time(1)
    for j in range(1, A):
        g_sent = lambda f: g_copy(0, j, f).wait_send()
        loop(0, RADIX, g_sent)
    loop(0, RADIX, lambda f: stage_out(1, f))

    for j in range(1, A):
        af_copy_in(j).wait_recv()
    total = by_af[0]
    for b in range(1, A):
        total = total + by_af[b]
    by_sa[s] = total
    for j in range(1, A):
        af_copy(j).wait_send()
    squares[...] = total

    def sa_copy(j):
        return remote(
            squares, by_sa.at[s], m_send.at[A + j], m_recv.at[A + j], (a, lax.rem(s + j, S))
        )

    def sa_copy_in(j):
        return remote(
            squares, by_sa.at[lax.rem(s + S - j, S)], m_send.at[A + j], m_recv.at[A + j], (a, lax.rem(s + j, S))
        )

    loop(1, S, lambda j: sa_copy(j).start())

    def sent(h):
        @pl.when(c + 1 < C)
        def _():
            loop(0, c + 1, lambda chip: up(chip, h).wait_send())

        @pl.when(c > 0)
        def _():
            loop(c, C, lambda chip: down(chip, h).wait_send())

        loop(0, C, lambda chip: across(chip, h).wait_send())

    loop(0, chunks, sent)
    for j in range(1, A):
        for part in range(2):
            initials(part, j).wait_send()
    loop(0, RADIX, h_sent)
    loop(1, S, lambda j: sa_copy_in(j).wait_recv())
    full = by_sa[0]
    for b in range(1, S):
        full = full + by_sa[b]
    mis[...] = full
    loop(1, S, lambda j: sa_copy(j).wait_send())

    def finish(f):
        for j in range(1, A):
            g_copy_in(1, j, f).wait_recv()
            g_copy(1, j, f).wait_send()

    loop(0, RADIX, finish)


def on_device(counts, data_real, data_imaginary, wave_real, wave_imaginary, primaries_real, primaries_imaginary):
    A, S = counts
    C = S // 2
    L, R, N = data_real.shape
    W = N // A
    U = L // RADIX
    chunks = RADIX if C <= 8 else 1
    turns = 2 * np.pi * np.arange(RADIX * RADIX) / (RADIX * RADIX)
    twiddle = jnp.asarray(np.stack([np.cos(turns), np.sin(turns)]), jnp.float32)
    smem = pl.BlockSpec(memory_space=pltpu.SMEM)
    hbm = pl.BlockSpec(memory_space=pl.ANY)
    vmem = pl.BlockSpec(memory_space=pltpu.VMEM)
    f32, bf16 = jnp.float32, jnp.bfloat16
    dma = pltpu.SemaphoreType.DMA
    split = lambda v: v.reshape(U, RADIX, R, N)
    coded, misfit = pl.pallas_call(
        functools.partial(kernel, A, S, chunks),
        in_specs=[smem, smem, smem, hbm, hbm, hbm, hbm],
        out_specs=[vmem, vmem],
        out_shape=[
            jax.ShapeDtypeStruct((2, U, RADIX, R, N), bf16),
            jax.ShapeDtypeStruct((ITERS, 8, 128), f32),
        ],
        scratch_shapes=[
            pltpu.VMEM((U, RADIX, 2, S, R, N), bf16),
            pltpu.VMEM((2, U, RADIX, R, N), f32),
            pltpu.VMEM((2, A, U, RADIX, R, W), f32),
            pltpu.VMEM((2, RADIX, RADIX, R, W), f32),
            pltpu.VMEM((2, RADIX, RADIX, R, W), f32),
            pltpu.VMEM((A, 2, U, RADIX, R, W), bf16),
            pltpu.VMEM((A, 2, U, RADIX, R, W), bf16),
            pltpu.VMEM((A, 2, U, RADIX, R, W), bf16),
            pltpu.VMEM((2, U, RADIX, R, N), bf16),
            pltpu.VMEM((ITERS, 8, 128), f32),
            pltpu.VMEM((A, ITERS, 8, 128), f32),
            pltpu.VMEM((S, ITERS, 8, 128), f32),
            dma((6,)),
            dma((C, chunks)),
            dma((C, chunks)),
            dma((C, chunks)),
            dma((C, chunks)),
            dma((C, chunks)),
            dma((2, A)),
            dma((2, A)),
            dma((A, RADIX)),
            dma((A, RADIX)),
            dma((ITERS, A, RADIX)),
            dma((ITERS, A, RADIX)),
            dma((A + S,)),
            dma((A + S,)),
        ],
        compiler_params=pltpu.CompilerParams(
            collective_id=0, has_side_effects=True, vmem_limit_bytes=63 * 2**20
        ),
    )(
        wave_real, wave_imaginary, twiddle,
        split(data_real), split(data_imaginary), split(primaries_real), split(primaries_imaginary),
    )
    updated = [decode(coded[part]).reshape(L, R, N) for part in range(2)]
    return (updated[0], updated[1], jnp.sum(misfit, axis=(1, 2)) / (L * A * N * N))


def solution(mesh):
    split = P("af", "sa", None)
    counts = (mesh.shape["af"], mesh.shape["sa"])
    return jax.shard_map(
        functools.partial(on_device, counts),
        mesh=mesh,
        in_specs=(split, split, P("af"), P("af"), split, split),
        out_specs=(split, split, P()),
        check_vma=False,
    )
```

```python
import functools
import math

import jax
import jax.numpy as jnp
import numpy as np
from jax import lax
from jax.experimental import pallas as pl
from jax.experimental.pallas import tpu as pltpu
from jax.sharding import PartitionSpec as P

ITERS = 2
STEP_LENGTH = 0.02
THRESHOLD = 0.25
RADIX = 8
LENT = 4
HALF = math.sqrt(0.5)
REACH = 64.0
TINY = 2.0**-126
MESH = pl.DeviceIdType.MESH


def encode(x):
    y = x * (1.0 / REACH)
    return ((y * y) * (y * jnp.abs(y))).astype(jnp.bfloat16)


def decode(code):
    v = code.astype(jnp.float32)
    r = lax.rsqrt(lax.rsqrt(jnp.maximum(jnp.abs(v), TINY))) * REACH
    return jnp.where(v > 0, r, jnp.where(v < 0, -r, 0.0))


def add(a, b):
    return (a[0] + b[0], a[1] + b[1])


def sub(a, b):
    return (a[0] - b[0], a[1] - b[1])


def turn(a, sign):
    return (-a[1], a[0]) if sign > 0 else (a[1], -a[0])


def rotate(a, c, s):
    return (a[0] * c - a[1] * s, a[0] * s + a[1] * c)


def four(a, b, c, d, sign):
    s0, s1, s2, s3 = add(a, c), sub(a, c), add(b, d), turn(sub(b, d), sign)
    return add(s0, s2), add(s1, s3), sub(s0, s2), sub(s1, s3)


def eight(x, sign):
    even = four(x[0], x[2], x[4], x[6], sign)
    odd = four(x[1], x[3], x[5], x[7], sign)
    o1 = add(odd[1], turn(odd[1], sign))
    o3 = sub(turn(odd[3], sign), odd[3])
    odd = (odd[0], (o1[0] * HALF, o1[1] * HALF), turn(odd[2], sign), (o3[0] * HALF, o3[1] * HALF))
    return [add(even[k], odd[k]) for k in range(4)] + [sub(even[k], odd[k]) for k in range(4)]


def shrink(v):
    return v - jnp.clip(v, -THRESHOLD, THRESHOLD)


def loop(start, stop, body):
    def step(i, _):
        body(i)
        return 0

    lax.fori_loop(start, stop, step, 0)


def kernel(
    A, S, chunks, lent, wr, wi, twiddle, data_r, data_i, prim_r, prim_i, out, mis,
    whole, current, initial, work, traces, hs, hr, gs, gr, squares, by_af, by_sa, lent_p, lent_g, lent_h,
    local_sem, up_sem, down_sem, ring_sem, pair_send, pair_recv,
    init_send, init_recv, h_send, h_recv, g_send, g_recv, m_send, m_recv,
    lp_send, lp_recv, lg_send, lg_recv, lh_send, lh_recv,
):
    C = S // 2
    U, _, R, N = data_r.shape
    W = N // A
    per = RADIX // chunks
    rows = 16 if R % 16 == 0 else 8
    a = lax.axis_index("af")
    s = lax.axis_index("sa")
    c = s // 2
    k = s % 2
    partner = c * 2 + 1 - k
    kept = chunks - lent
    F0 = kept * per
    Q = RADIX - F0
    if lent:
        is_end = (c == 0) | (c == C - 1)
        is_helper = (c == 1) | (c == C - 2)
        other = jnp.where((c == 0) | (c == C - 2), s + 2, s - 2)

    def goes_up(h):
        go = c + 1 < C
        return go & ((h < kept) | (c + 2 < C)) if lent else go

    def goes_down(h):
        go = c > 0
        return go & ((h < kept) | (c > 1)) if lent else go

    def keeps(h):
        return (h < kept) | jnp.logical_not(is_end) if lent else h >= 0

    mine = pl.ds(pl.multiple_of(a * W, W), W)

    def cols(b):
        return pl.ds(pl.multiple_of(b * W, W), W)

    def ahead(j):
        return lax.rem(a + j, A)

    def behind(j):
        return lax.rem(a + A - j, A)

    barrier = pltpu.get_barrier_semaphore()
    for j in range(1, A):
        pl.semaphore_signal(barrier, inc=1, device_id=(ahead(j), s), device_id_type=MESH)
    loop(
        1, S,
        lambda j: pl.semaphore_signal(barrier, inc=1, device_id=(a, lax.rem(s + j, S)), device_id_type=MESH),
    )

    locals_ = [
        pltpu.make_async_copy(data_r, whole.at[:, :, 0, s], local_sem.at[0]),
        pltpu.make_async_copy(data_i, whole.at[:, :, 1, s], local_sem.at[1]),
        pltpu.make_async_copy(prim_r, current.at[0], local_sem.at[2]),
        pltpu.make_async_copy(prim_i, current.at[1], local_sem.at[3]),
        pltpu.make_async_copy(prim_r.at[:, :, :, mine], initial.at[0, a], local_sem.at[4]),
        pltpu.make_async_copy(prim_i.at[:, :, :, mine], initial.at[1, a], local_sem.at[5]),
    ]
    for copy in locals_:
        copy.start()
    squares[...] = jnp.zeros_like(squares)
    pl.semaphore_wait(barrier, A - 1 + S - 1)

    def shard(chip, core, h):
        return whole.at[:, pl.ds(h * per, per), :, chip * 2 + core]

    def remote(src, dst, send, recv, device):
        return pltpu.make_async_remote_copy(
            src_ref=src, dst_ref=dst, send_sem=send, recv_sem=recv, device_id=device, device_id_type=MESH
        )

    def up(chip, h):
        ref = shard(chip, k, h)
        return remote(ref, ref, up_sem.at[chip, h], ring_sem.at[chip, h], (a, lax.rem(s + 2, S)))

    def down(chip, h):
        ref = shard(chip, k, h)
        return remote(ref, ref, down_sem.at[chip, h], ring_sem.at[chip, h], (a, lax.rem(s + S - 2, S)))

    def across(chip, h):
        ref = shard(chip, k, h)
        return remote(ref, ref, pair_send.at[chip, h], pair_recv.at[chip, h], (a, partner))

    def across_in(chip, h):
        ref = shard(chip, 1 - k, h)
        return remote(ref, ref, pair_send.at[chip, h], pair_recv.at[chip, h], (a, partner))

    def initials(part, j):
        src = (prim_r, prim_i)[part]
        return remote(
            src.at[:, :, :, cols(ahead(j))], initial.at[part, a],
            init_send.at[part, j], init_recv.at[part, j], (ahead(j), s),
        )

    def initials_in(part, j):
        src = (prim_r, prim_i)[part]
        return remote(
            src.at[:, :, :, mine], initial.at[part, behind(j)],
            init_send.at[part, j], init_recv.at[part, j], (ahead(j), s),
        )

    locals_[0].wait()
    locals_[1].wait()

    def first(h):
        @pl.when(goes_up(h))
        def _():
            up(c, h).start()

        @pl.when(goes_down(h))
        def _():
            down(c, h).start()

        @pl.when(keeps(h))
        def _():
            across(c, h).start()

    loop(0, chunks, first)

    def lend_p(part, n):
        src = (prim_r, prim_i)[part]
        return remote(
            src.at[:, F0 + n], lent_p.at[part, :, n], lp_send.at[part, n], lp_recv.at[part, n], (a, other)
        )

    def lend_g(n):
        return remote(gr.at[:, :, F0 + n], lent_g.at[:, :, n], lg_send.at[n], lg_recv.at[n], (a, other))

    def lend_h(n):
        return remote(lent_h.at[:, :, :, n], hs.at[:, :, :, F0 + n], lh_send.at[n], lh_recv.at[n], (a, other))

    if lent:

        @pl.when(is_end)
        def _():
            def lend(n):
                lend_p(0, n).start()
                lend_p(1, n).start()

            loop(0, Q, lend)

    for j in range(1, A):
        for part in range(2):
            initials(part, j).start()

    def arrive(d, h):
        @pl.when(c >= d)
        def _():
            src = c - d
            up(src, h).wait_recv()
            across(src, h).start()

            @pl.when(goes_up(h))
            def _():
                up(src, h).start()

        @pl.when(c + d < C)
        def _():
            src = c + d
            down(src, h).wait_recv()
            across(src, h).start()

            @pl.when(goes_down(h))
            def _():
                down(src, h).start()

    far = jnp.maximum(c, C - 1 - c)

    def pass_on(h, d):
        @pl.when(keeps(h))
        def _():
            arrive(d, h)

    loop(1, far, lambda d: loop(0, chunks, lambda h: pass_on(h, d)))

    def h_copy(j, f):
        to = ahead(j)
        return remote(
            hs.at[to, :, :, f], hr.at[a, :, :, f], h_send.at[j, f], h_recv.at[j, f], (to, s)
        )

    def h_copy_in(j, f):
        return remote(
            hs.at[a, :, :, f], hr.at[behind(j), :, :, f], h_send.at[j, f], h_recv.at[j, f], (ahead(j), s)
        )

    def g_copy(it, j, f):
        to = ahead(j)
        dst = gr if it == 0 else out
        return remote(
            gs.at[to, :, :, f], dst.at[:, :, f, :, mine],
            g_send.at[it, j, f], g_recv.at[it, j, f], (to, s),
        )

    def g_copy_in(it, j, f):
        dst = gr if it == 0 else out
        return remote(
            gs.at[a, :, :, f], dst.at[:, :, f, :, cols(behind(j))],
            g_send.at[it, j, f], g_recv.at[it, j, f], (ahead(j), s),
        )

    def step_of(it, f, u, at, re, im):
        qr = wr[u * RADIX + f]
        qi = wi[u * RADIX + f]
        whole_r = whole[u, f, 0].reshape(N, N)
        whole_i = whole[u, f, 1].reshape(N, N)
        left = jnp.concatenate([re.astype(jnp.bfloat16), im.astype(jnp.bfloat16)], axis=0)
        pr = jnp.dot(left, whole_r, preferred_element_type=jnp.float32)
        pi = jnp.dot(left, whole_i, preferred_element_type=jnp.float32)
        er = whole[u, f, 0, at].astype(jnp.float32) + (pr[:R] - pi[R:]) - (qr * re - qi * im)
        ei = whole[u, f, 1, at].astype(jnp.float32) + (pi[:R] + pr[R:]) - (qr * im + qi * re)
        sq = er * er + ei * ei
        part = sq[:8]
        for i in range(1, R // 8):
            part = part + sq[i * 8 : (i + 1) * 8]
        row = part[:, :128]
        for i in range(1, N // 128):
            row = row + part[:, i * 128 : (i + 1) * 128]
        squares[it] += row
        eb = jnp.concatenate([er.astype(jnp.bfloat16), ei.astype(jnp.bfloat16)], axis=0)
        dims = (((1,), (1,)), ((), ()))
        br = lax.dot_general(eb, whole_r, dims, preferred_element_type=jnp.float32)
        bi = lax.dot_general(eb, whole_i, dims, preferred_element_type=jnp.float32)
        dr = encode(STEP_LENGTH * (qr * er + qi * ei - (br[:R] + bi[R:])))
        di = encode(STEP_LENGTH * (qr * ei - qi * er - (br[R:] - bi[:R])))
        return dr, di

    def publish(f):
        for u in range(U):
            hr[a, 0, u, f] = hs[a, 0, u, f]
            hr[a, 1, u, f] = hs[a, 1, u, f]
        for j in range(1, A):
            h_copy(j, f).start()

    def product(it, f):
        def one(u):
            if it == 0:
                re = current[0, u, f]
                im = current[1, u, f]
            else:
                re = gr[0, u, f].astype(jnp.float32)
                im = gr[1, u, f].astype(jnp.float32)
            dr, di = step_of(it, f, u, s, re, im)
            for b in range(A):
                hs[b, 0, u, f] = dr[:, b * W : (b + 1) * W]
                hs[b, 1, u, f] = di[:, b * W : (b + 1) * W]

        loop(0, U, one)
        publish(f)

    def lent_product(it, n):
        if it == 0:
            lend_p(0, n).wait_recv()
            lend_p(1, n).wait_recv()
        else:
            lend_g(n).wait_recv()
            lend_h(n).wait_send()

        def one(u):
            if it == 0:
                re = lent_p[0, u, n]
                im = lent_p[1, u, n]
            else:
                re = lent_g[0, u, n].astype(jnp.float32)
                im = lent_g[1, u, n].astype(jnp.float32)
            dr, di = step_of(it, F0 + n, u, other, re, im)
            for b in range(A):
                lent_h[b, 0, u, n] = dr[:, b * W : (b + 1) * W]
                lent_h[b, 1, u, n] = di[:, b * W : (b + 1) * W]

        loop(0, U, one)
        lend_h(n).start()

    def returned(n):
        lend_h(n).wait_recv()
        publish(F0 + n)

    def stage_in(it, f):
        for j in range(1, A):
            h_copy_in(j, f).wait_recv()

        def some(g):
            at = pl.ds(pl.multiple_of(g * rows, rows), rows)
            x = []
            for f2 in range(RADIX):
                b, u = divmod(f2, U)
                re = decode(hr[b, 0, u, f, at, :])
                im = decode(hr[b, 1, u, f, at, :])
                if it == 0:
                    re = re + initial[0, b, u, f, at, :]
                    im = im + initial[1, b, u, f, at, :]
                x.append((re * (1.0 / RADIX), im * (1.0 / RADIX)))
            y = eight(x, 1)
            for t in range(RADIX):
                v = rotate(y[t], twiddle[0, f * t], twiddle[1, f * t]) if t else y[t]
                work[0, f, t, at, :] = v[0]
                work[1, f, t, at, :] = v[1]

        loop(0, R // rows, some)

    def stage_time(it):
        def some(g):
            at = pl.ds(pl.multiple_of(g * rows, rows), rows)

            def one(t):
                y = eight([(work[0, f, t, at, :], work[1, f, t, at, :]) for f in range(RADIX)], 1)
                if it > 0:
                    y = [(v[0] + traces[0, n, t, at, :], v[1] + traces[1, n, t, at, :]) for n, v in enumerate(y)]
                y = [(shrink(v[0]), shrink(v[1])) for v in y]
                if it < ITERS - 1:
                    for n, v in enumerate(y):
                        traces[0, n, t, at, :] = v[0]
                        traces[1, n, t, at, :] = v[1]
                y = eight(y, -1)
                for f in range(RADIX):
                    v = rotate(y[f], twiddle[0, f * t], -twiddle[1, f * t]) if f else y[f]
                    work[0, f, t, at, :] = v[0]
                    work[1, f, t, at, :] = v[1]

            loop(0, RADIX, one)

        loop(0, R // rows, some)

    def stage_out(it, f):
        dst = gr if it == 0 else out

        def some(g):
            at = pl.ds(pl.multiple_of(g * rows, rows), rows)
            y = eight([(work[0, f, t, at, :], work[1, f, t, at, :]) for t in range(RADIX)], -1)
            for f2 in range(RADIX):
                b, u = divmod(f2, U)
                for part in range(2):
                    v = y[f2][part] * (1.0 / RADIX)
                    gs[b, part, u, f, at, :] = v.astype(jnp.bfloat16) if it == 0 else encode(v)

        loop(0, R // rows, some)
        for j in range(1, A):
            g_copy(it, j, f).start()
        for part in range(2):
            for u in range(U):
                dst[part, u, f, :, mine] = gs[a, part, u, f]

    for copy in locals_[2:]:
        copy.wait()
    for j in range(1, A):
        for part in range(2):
            initials_in(part, j).wait_recv()

    def last(h):
        @pl.when(keeps(h))
        def _():
            arrive(far, h)
            loop(0, C, lambda chip: across_in(chip, h).wait_recv())

        if lent:

            @pl.when(is_helper & (h >= kept))
            def _():
                loop(0, per, lambda i: lent_product(0, (h - kept) * per + i))

            @pl.when(is_end & (h >= kept))
            def _():
                loop(0, per, lambda i: returned((h - kept) * per + i))

        @pl.when(keeps(h))
        def _():
            loop(0, per, lambda i: product(0, h * per + i))

        @pl.when(h > 0)
        def _():
            loop(0, per, lambda i: stage_in(0, (h - 1) * per + i))

    loop(0, chunks, last)
    loop(0, per, lambda i: stage_in(0, (chunks - 1) * per + i))
    stage_time(0)
    order = lambda i: lax.rem(F0 + i, RADIX)
    loop(0, RADIX, lambda i: stage_out(0, order(i)))

    def h_sent(f):
        for j in range(1, A):
            h_copy(j, f).wait_send()

    loop(0, RADIX, h_sent)

    def lends(f):
        return is_end & (f >= F0)

    def again(i):
        f = order(i)
        for j in range(1, A):
            g_copy_in(0, j, f).wait_recv()
        if lent:

            @pl.when(lends(f))
            def _():
                lend_g(f - F0).start()

            @pl.when(jnp.logical_not(lends(f)))
            def _():
                product(1, f)

            @pl.when(is_helper & (i >= 2) & (lax.rem(i, 2) == 0) & (i < 2 * Q + 2))
            def _():
                lent_product(1, i // 2 - 1)

            before = order(i + RADIX - 1)

            @pl.when((i > 0) & jnp.logical_not(lends(before)))
            def _():
                stage_in(1, before)

        else:
            product(1, f)

            @pl.when(i > 0)
            def _():
                stage_in(1, order(i + RADIX - 1))

    loop(0, RADIX, again)
    if lent:
        late = (RADIX - 1) // 2

        @pl.when(is_helper)
        def _():
            if late < Q:
                loop(late, Q, lambda n: lent_product(1, n))

        @pl.when(is_end)
        def _():
            loop(0, Q, returned)

    by_af[a] = squares[...]

    def af_copy(j):
        return remote(squares, by_af.at[a], m_send.at[j], m_recv.at[j], (ahead(j), s))

    def af_copy_in(j):
        return remote(squares, by_af.at[behind(j)], m_send.at[j], m_recv.at[j], (ahead(j), s))

    for j in range(1, A):
        af_copy(j).start()
    stage_in(1, order(RADIX - 1))
    if lent:

        @pl.when(is_end)
        def _():
            loop(0, Q, lambda n: stage_in(1, F0 + n))

    stage_time(1)
    for j in range(1, A):
        g_sent = lambda f: g_copy(0, j, f).wait_send()
        loop(0, RADIX, g_sent)
    loop(0, RADIX, lambda f: stage_out(1, f))

    for j in range(1, A):
        af_copy_in(j).wait_recv()
    total = by_af[0]
    for b in range(1, A):
        total = total + by_af[b]
    by_sa[s] = total
    for j in range(1, A):
        af_copy(j).wait_send()
    squares[...] = total

    def sa_copy(j):
        return remote(
            squares, by_sa.at[s], m_send.at[A + j], m_recv.at[A + j], (a, lax.rem(s + j, S))
        )

    def sa_copy_in(j):
        return remote(
            squares, by_sa.at[lax.rem(s + S - j, S)], m_send.at[A + j], m_recv.at[A + j], (a, lax.rem(s + j, S))
        )

    loop(1, S, lambda j: sa_copy(j).start())

    def sent(h):
        @pl.when(goes_up(h))
        def _():
            loop(0, c + 1, lambda chip: up(chip, h).wait_send())

        @pl.when(goes_down(h))
        def _():
            loop(c, C, lambda chip: down(chip, h).wait_send())

        @pl.when(keeps(h))
        def _():
            loop(0, C, lambda chip: across(chip, h).wait_send())

    loop(0, chunks, sent)
    if lent:

        @pl.when(is_end)
        def _():
            def lent_out(n):
                lend_p(0, n).wait_send()
                lend_p(1, n).wait_send()
                lend_g(n).wait_send()

            loop(0, Q, lent_out)

        @pl.when(is_helper)
        def _():
            loop(0, Q, lambda n: lend_h(n).wait_send())

    for j in range(1, A):
        for part in range(2):
            initials(part, j).wait_send()
    loop(0, RADIX, h_sent)
    loop(1, S, lambda j: sa_copy_in(j).wait_recv())
    full = by_sa[0]
    for b in range(1, S):
        full = full + by_sa[b]
    mis[...] = full
    loop(1, S, lambda j: sa_copy(j).wait_send())

    def finish(f):
        for j in range(1, A):
            g_copy_in(1, j, f).wait_recv()
            g_copy(1, j, f).wait_send()

    loop(0, RADIX, finish)


def on_device(counts, data_real, data_imaginary, wave_real, wave_imaginary, primaries_real, primaries_imaginary):
    A, S = counts
    C = S // 2
    L, R, N = data_real.shape
    W = N // A
    U = L // RADIX
    chunks = RADIX if C <= 8 else 1
    lent = LENT if C >= 4 and chunks > LENT else 0
    Q = max(1, lent * RADIX // chunks)
    turns = 2 * np.pi * np.arange(RADIX * RADIX) / (RADIX * RADIX)
    twiddle = jnp.asarray(np.stack([np.cos(turns), np.sin(turns)]), jnp.float32)
    smem = pl.BlockSpec(memory_space=pltpu.SMEM)
    hbm = pl.BlockSpec(memory_space=pl.ANY)
    vmem = pl.BlockSpec(memory_space=pltpu.VMEM)
    f32, bf16 = jnp.float32, jnp.bfloat16
    dma = pltpu.SemaphoreType.DMA
    split = lambda v: v.reshape(U, RADIX, R, N)
    coded, misfit = pl.pallas_call(
        functools.partial(kernel, A, S, chunks, lent),
        in_specs=[smem, smem, smem, hbm, hbm, hbm, hbm],
        out_specs=[vmem, vmem],
        out_shape=[
            jax.ShapeDtypeStruct((2, U, RADIX, R, N), bf16),
            jax.ShapeDtypeStruct((ITERS, 8, 128), f32),
        ],
        scratch_shapes=[
            pltpu.VMEM((U, RADIX, 2, S, R, N), bf16),
            pltpu.VMEM((2, U, RADIX, R, N), f32),
            pltpu.VMEM((2, A, U, RADIX, R, W), f32),
            pltpu.VMEM((2, RADIX, RADIX, R, W), f32),
            pltpu.VMEM((2, RADIX, RADIX, R, W), f32),
            pltpu.VMEM((A, 2, U, RADIX, R, W), bf16),
            pltpu.VMEM((A, 2, U, RADIX, R, W), bf16),
            pltpu.VMEM((A, 2, U, RADIX, R, W), bf16),
            pltpu.VMEM((2, U, RADIX, R, N), bf16),
            pltpu.VMEM((ITERS, 8, 128), f32),
            pltpu.VMEM((A, ITERS, 8, 128), f32),
            pltpu.VMEM((S, ITERS, 8, 128), f32),
            pltpu.VMEM((2, U, Q, R, N), f32),
            pltpu.VMEM((2, U, Q, R, N), bf16),
            pltpu.VMEM((A, 2, U, Q, R, W), bf16),
            dma((6,)),
            dma((C, chunks)),
            dma((C, chunks)),
            dma((C, chunks)),
            dma((C, chunks)),
            dma((C, chunks)),
            dma((2, A)),
            dma((2, A)),
            dma((A, RADIX)),
            dma((A, RADIX)),
            dma((ITERS, A, RADIX)),
            dma((ITERS, A, RADIX)),
            dma((A + S,)),
            dma((A + S,)),
            dma((2, Q)),
            dma((2, Q)),
            dma((Q,)),
            dma((Q,)),
            dma((Q,)),
            dma((Q,)),
        ],
        compiler_params=pltpu.CompilerParams(
            collective_id=0, has_side_effects=True, vmem_limit_bytes=63 * 2**20
        ),
    )(
        wave_real, wave_imaginary, twiddle,
        split(data_real), split(data_imaginary), split(primaries_real), split(primaries_imaginary),
    )
    updated = [decode(coded[part]).reshape(L, R, N) for part in range(2)]
    return (updated[0], updated[1], jnp.sum(misfit, axis=(1, 2)) / (L * A * N * N))


def solution(mesh):
    split = P("af", "sa", None)
    counts = (mesh.shape["af"], mesh.shape["sa"])
    return jax.shard_map(
        functools.partial(on_device, counts),
        mesh=mesh,
        in_specs=(split, split, P("af"), P("af"), split, split),
        out_specs=(split, split, P()),
        check_vma=False,
    )
```

```python
import functools
import math

import jax
import jax.numpy as jnp
import numpy as np
from jax import lax
from jax.experimental import pallas as pl
from jax.experimental.pallas import tpu as pltpu
from jax.sharding import PartitionSpec as P

ITERS = 2
STEP_LENGTH = 0.02
THRESHOLD = 0.25
RADIX = 8
LENT = 3
HALF = math.sqrt(0.5)
REACH = 64.0
TINY = 2.0**-126
MESH = pl.DeviceIdType.MESH


def encode(x):
    y = x * (1.0 / REACH)
    return ((y * y) * (y * jnp.abs(y))).astype(jnp.bfloat16)


def decode(code):
    v = code.astype(jnp.float32)
    y = lax.rsqrt(jnp.maximum(jnp.abs(v), TINY))
    return ((v * y) * y) * (lax.rsqrt(y) * REACH)


def add(a, b):
    return (a[0] + b[0], a[1] + b[1])


def sub(a, b):
    return (a[0] - b[0], a[1] - b[1])


def turn(a, sign):
    return (-a[1], a[0]) if sign > 0 else (a[1], -a[0])


def rotate(a, c, s):
    return (a[0] * c - a[1] * s, a[0] * s + a[1] * c)


def four(a, b, c, d, sign):
    s0, s1, s2, s3 = add(a, c), sub(a, c), add(b, d), turn(sub(b, d), sign)
    return add(s0, s2), add(s1, s3), sub(s0, s2), sub(s1, s3)


def eight(x, sign):
    even = four(x[0], x[2], x[4], x[6], sign)
    odd = four(x[1], x[3], x[5], x[7], sign)
    o1 = add(odd[1], turn(odd[1], sign))
    o3 = sub(turn(odd[3], sign), odd[3])
    odd = (odd[0], (o1[0] * HALF, o1[1] * HALF), turn(odd[2], sign), (o3[0] * HALF, o3[1] * HALF))
    return [add(even[k], odd[k]) for k in range(4)] + [sub(even[k], odd[k]) for k in range(4)]


def shrink(v):
    return v - jnp.clip(v, -THRESHOLD, THRESHOLD)


def loop(start, stop, body):
    def step(i, _):
        body(i)
        return 0

    lax.fori_loop(start, stop, step, 0)


def kernel(
    A, S, chunks, lent, wr, wi, twiddle, data_r, data_i, prim_r, prim_i, out, mis,
    whole, current, initial, work, traces, hs, hr, gs, gr, squares, by_af, by_sa, lent_g, lent_h,
    local_sem, up_sem, down_sem, ring_sem, pair_send, pair_recv,
    init_send, init_recv, h_send, h_recv, g_send, g_recv, m_send, m_recv,
    lg_send, lg_recv, lh_send, lh_recv, out_sem,
):
    C = S // 2
    U, _, R, N = data_r.shape
    W = N // A
    per = RADIX // chunks
    rows = 16 if R % 16 == 0 else 8
    a = lax.axis_index("af")
    s = lax.axis_index("sa")
    c = s // 2
    k = s % 2
    partner = c * 2 + 1 - k
    kept = chunks - lent
    F0 = kept * per
    Q = RADIX - F0
    if lent:
        is_end = (c == 0) | (c == C - 1)
        is_helper = (c == 1) | (c == C - 2)
        other = jnp.where((c == 0) | (c == C - 2), s + 2, s - 2)

    def goes_up(h):
        go = c + 1 < C
        return go & ((h < kept) | (c + 2 < C)) if lent else go

    def goes_down(h):
        go = c > 0
        return go & ((h < kept) | (c > 1)) if lent else go

    def keeps(h):
        return (h < kept) | jnp.logical_not(is_end) if lent else h >= 0

    mine = pl.ds(pl.multiple_of(a * W, W), W)

    def cols(b):
        return pl.ds(pl.multiple_of(b * W, W), W)

    def ahead(j):
        return lax.rem(a + j, A)

    def behind(j):
        return lax.rem(a + A - j, A)

    barrier = pltpu.get_barrier_semaphore()
    for j in range(1, A):
        pl.semaphore_signal(barrier, inc=1, device_id=(ahead(j), s), device_id_type=MESH)
    loop(
        1, S,
        lambda j: pl.semaphore_signal(barrier, inc=1, device_id=(a, lax.rem(s + j, S)), device_id_type=MESH),
    )

    locals_ = [
        pltpu.make_async_copy(data_r, whole.at[:, :, 0, s], local_sem.at[0]),
        pltpu.make_async_copy(data_i, whole.at[:, :, 1, s], local_sem.at[1]),
        pltpu.make_async_copy(prim_r, current.at[0], local_sem.at[2]),
        pltpu.make_async_copy(prim_i, current.at[1], local_sem.at[3]),
        pltpu.make_async_copy(prim_r.at[:, :, :, mine], initial.at[0, a], local_sem.at[4]),
        pltpu.make_async_copy(prim_i.at[:, :, :, mine], initial.at[1, a], local_sem.at[5]),
    ]
    squares[...] = jnp.zeros_like(squares)
    pl.semaphore_wait(barrier, A - 1 + S - 1)

    def shard(chip, core, h):
        return whole.at[:, pl.ds(h * per, per), :, chip * 2 + core]

    def remote(src, dst, send, recv, device):
        return pltpu.make_async_remote_copy(
            src_ref=src, dst_ref=dst, send_sem=send, recv_sem=recv, device_id=device, device_id_type=MESH
        )

    def own(part, h):
        return (data_r, data_i)[part].at[:, pl.ds(h * per, per)]

    def up(chip, h):
        ref = shard(chip, k, h)
        return remote(ref, ref, up_sem.at[chip, h], ring_sem.at[chip, h], (a, lax.rem(s + 2, S)))

    def down(chip, h):
        ref = shard(chip, k, h)
        return remote(ref, ref, down_sem.at[chip, h], ring_sem.at[chip, h], (a, lax.rem(s + S - 2, S)))

    def across(chip, h):
        ref = shard(chip, k, h)
        return remote(ref, ref, pair_send.at[chip, h], pair_recv.at[chip, h], (a, partner))

    def own_up(part, h):
        return remote(
            own(part, h), shard(c, k, h).at[:, :, part], up_sem.at[c, h], ring_sem.at[c, h], (a, lax.rem(s + 2, S))
        )

    def own_down(part, h):
        return remote(
            own(part, h), shard(c, k, h).at[:, :, part], down_sem.at[c, h], ring_sem.at[c, h], (a, lax.rem(s + S - 2, S))
        )

    def own_across(part, h):
        return remote(
            own(part, h), shard(c, k, h).at[:, :, part], pair_send.at[c, h], pair_recv.at[c, h], (a, partner)
        )

    def across_in(chip, h):
        ref = shard(chip, 1 - k, h)
        return remote(ref, ref, pair_send.at[chip, h], pair_recv.at[chip, h], (a, partner))

    def initials(part, j):
        src = (prim_r, prim_i)[part]
        return remote(
            src.at[:, :, :, cols(ahead(j))], initial.at[part, a],
            init_send.at[part, j], init_recv.at[part, j], (ahead(j), s),
        )

    def initials_in(part, j):
        src = (prim_r, prim_i)[part]
        return remote(
            src.at[:, :, :, mine], initial.at[part, behind(j)],
            init_send.at[part, j], init_recv.at[part, j], (ahead(j), s),
        )

    def first(h):
        @pl.when(goes_up(h))
        def _():
            own_up(0, h).start()
            own_up(1, h).start()

        @pl.when(goes_down(h))
        def _():
            own_down(0, h).start()
            own_down(1, h).start()

        @pl.when(keeps(h))
        def _():
            own_across(0, h).start()
            own_across(1, h).start()

    loop(0, chunks, first)

    def lend_g(n):
        return remote(gr.at[:, :, F0 + n], lent_g.at[:, :, n], lg_send.at[n], lg_recv.at[n], (a, other))

    def lend_h(n):
        return remote(lent_h.at[:, :, :, n], hs.at[:, :, :, F0 + n], lh_send.at[n], lh_recv.at[n], (a, other))

    for j in range(1, A):
        for part in range(2):
            initials(part, j).start()
    for copy in locals_:
        copy.start()
    for copy in locals_[2:4]:
        copy.wait()
    if lent:

        @pl.when(is_end)
        def _():
            def lend(n):
                for part in range(2):
                    for u in range(U):
                        gr[part, u, F0 + n] = current[part, u, F0 + n].astype(jnp.bfloat16)
                lend_g(n).start()

            loop(0, Q, lend)


    def arrive(d, h):
        @pl.when(c >= d)
        def _():
            src = c - d
            up(src, h).wait_recv()
            across(src, h).start()

            @pl.when(goes_up(h))
            def _():
                up(src, h).start()

        @pl.when(c + d < C)
        def _():
            src = c + d
            down(src, h).wait_recv()
            across(src, h).start()

            @pl.when(goes_down(h))
            def _():
                down(src, h).start()

    far = jnp.maximum(c, C - 1 - c)

    def pass_on(h, d):
        @pl.when(keeps(h))
        def _():
            arrive(d, h)

    loop(1, far, lambda d: loop(0, chunks, lambda h: pass_on(h, d)))

    def h_copy(j, f):
        to = ahead(j)
        return remote(
            hs.at[to, :, :, f], hr.at[a, :, :, f], h_send.at[j, f], h_recv.at[j, f], (to, s)
        )

    def h_copy_in(j, f):
        return remote(
            hs.at[a, :, :, f], hr.at[behind(j), :, :, f], h_send.at[j, f], h_recv.at[j, f], (ahead(j), s)
        )

    def g_copy(it, j, f):
        to = ahead(j)
        dst = gr if it == 0 else out
        return remote(
            gs.at[to, :, :, f], dst.at[:, :, f, :, mine],
            g_send.at[it, j, f], g_recv.at[it, j, f], (to, s),
        )

    def g_copy_in(it, j, f):
        dst = gr if it == 0 else out
        return remote(
            gs.at[a, :, :, f], dst.at[:, :, f, :, cols(behind(j))],
            g_send.at[it, j, f], g_recv.at[it, j, f], (ahead(j), s),
        )

    def step_of(it, f, u, at, re, im):
        qr = wr[u * RADIX + f]
        qi = wi[u * RADIX + f]
        whole_r = whole[u, f, 0].reshape(N, N)
        whole_i = whole[u, f, 1].reshape(N, N)
        left = jnp.concatenate([re.astype(jnp.bfloat16), im.astype(jnp.bfloat16)], axis=0)
        pr = jnp.dot(left, whole_r, preferred_element_type=jnp.float32)
        pi = jnp.dot(left, whole_i, preferred_element_type=jnp.float32)
        er = whole[u, f, 0, at].astype(jnp.float32) + (pr[:R] - pi[R:]) - (qr * re - qi * im)
        ei = whole[u, f, 1, at].astype(jnp.float32) + (pi[:R] + pr[R:]) - (qr * im + qi * re)
        sq = er * er + ei * ei
        part = sq[:8]
        for i in range(1, R // 8):
            part = part + sq[i * 8 : (i + 1) * 8]
        row = part[:, :128]
        for i in range(1, N // 128):
            row = row + part[:, i * 128 : (i + 1) * 128]
        squares[it] += row
        eb = jnp.concatenate([er.astype(jnp.bfloat16), ei.astype(jnp.bfloat16)], axis=0)
        dims = (((1,), (1,)), ((), ()))
        br = lax.dot_general(eb, whole_r, dims, preferred_element_type=jnp.float32)
        bi = lax.dot_general(eb, whole_i, dims, preferred_element_type=jnp.float32)
        dr = encode(STEP_LENGTH * (qr * er + qi * ei - (br[:R] + bi[R:])))
        di = encode(STEP_LENGTH * (qr * ei - qi * er - (br[R:] - bi[:R])))
        return dr, di

    def publish(f):
        for u in range(U):
            hr[a, 0, u, f] = hs[a, 0, u, f]
            hr[a, 1, u, f] = hs[a, 1, u, f]
        for j in range(1, A):
            h_copy(j, f).start()

    def product(it, f):
        def one(u):
            if it == 0:
                re = current[0, u, f]
                im = current[1, u, f]
            else:
                re = gr[0, u, f].astype(jnp.float32)
                im = gr[1, u, f].astype(jnp.float32)
            dr, di = step_of(it, f, u, s, re, im)
            for b in range(A):
                hs[b, 0, u, f] = dr[:, b * W : (b + 1) * W]
                hs[b, 1, u, f] = di[:, b * W : (b + 1) * W]

        loop(0, U, one)
        publish(f)

    def lent_product(it, n):
        lend_g(n).wait_recv()
        if it > 0:
            lend_h(n).wait_send()

        def one(u):
            re = lent_g[0, u, n].astype(jnp.float32)
            im = lent_g[1, u, n].astype(jnp.float32)
            dr, di = step_of(it, F0 + n, u, other, re, im)
            for b in range(A):
                lent_h[b, 0, u, n] = dr[:, b * W : (b + 1) * W]
                lent_h[b, 1, u, n] = di[:, b * W : (b + 1) * W]

        loop(0, U, one)
        lend_h(n).start()

    def returned(n):
        lend_h(n).wait_recv()
        lend_g(n).wait_send()
        publish(F0 + n)

    def stage_in(it, f):
        for j in range(1, A):
            h_copy_in(j, f).wait_recv()

        def some(g):
            at = pl.ds(pl.multiple_of(g * rows, rows), rows)
            x = []
            for f2 in range(RADIX):
                b, u = divmod(f2, U)
                re = decode(hr[b, 0, u, f, at, :])
                im = decode(hr[b, 1, u, f, at, :])
                if it == 0:
                    re = re + initial[0, b, u, f, at, :]
                    im = im + initial[1, b, u, f, at, :]
                x.append((re * (1.0 / RADIX), im * (1.0 / RADIX)))
            y = eight(x, 1)
            for t in range(RADIX):
                v = rotate(y[t], twiddle[0, f * t], twiddle[1, f * t]) if t else y[t]
                work[0, f, t, at, :] = v[0]
                work[1, f, t, at, :] = v[1]

        loop(0, R // rows, some)

    def stage_time(it):
        def some(g):
            at = pl.ds(pl.multiple_of(g * rows, rows), rows)

            def one(t):
                y = eight([(work[0, f, t, at, :], work[1, f, t, at, :]) for f in range(RADIX)], 1)
                if it > 0:
                    y = [(v[0] + traces[0, n, t, at, :], v[1] + traces[1, n, t, at, :]) for n, v in enumerate(y)]
                y = [(shrink(v[0]), shrink(v[1])) for v in y]
                if it < ITERS - 1:
                    for n, v in enumerate(y):
                        traces[0, n, t, at, :] = v[0]
                        traces[1, n, t, at, :] = v[1]
                y = eight(y, -1)
                for f in range(RADIX):
                    v = rotate(y[f], twiddle[0, f * t], -twiddle[1, f * t]) if f else y[f]
                    work[0, f, t, at, :] = v[0]
                    work[1, f, t, at, :] = v[1]

            loop(0, RADIX, one)

        loop(0, R // rows, some)

    def own_out(f):
        return pltpu.make_async_copy(gs.at[a, :, :, f], out.at[:, :, f, :, mine], out_sem.at[f])

    def stage_out(it, f):
        def some(g):
            at = pl.ds(pl.multiple_of(g * rows, rows), rows)
            y = eight([(work[0, f, t, at, :], work[1, f, t, at, :]) for t in range(RADIX)], -1)
            for f2 in range(RADIX):
                b, u = divmod(f2, U)
                for part in range(2):
                    v = y[f2][part] * (1.0 / RADIX)
                    gs[b, part, u, f, at, :] = v.astype(jnp.bfloat16) if it == 0 else encode(v)

        loop(0, R // rows, some)
        for j in range(1, A):
            g_copy(it, j, f).start()
        if it == 0:
            for part in range(2):
                for u in range(U):
                    gr[part, u, f, :, mine] = gs[a, part, u, f]
        else:
            own_out(f).start()

    for copy in locals_[:2] + locals_[4:]:
        copy.wait()
    for j in range(1, A):
        for part in range(2):
            initials_in(part, j).wait_recv()

    def last(h):
        @pl.when(keeps(h))
        def _():
            arrive(far, h)
            loop(0, C, lambda chip: across_in(chip, h).wait_recv())

        if lent:

            @pl.when(is_helper & (h >= kept))
            def _():
                loop(0, per, lambda i: lent_product(0, (h - kept) * per + i))

            @pl.when(is_end & (h >= kept))
            def _():
                loop(0, per, lambda i: returned((h - kept) * per + i))

        @pl.when(keeps(h))
        def _():
            loop(0, per, lambda i: product(0, h * per + i))

        @pl.when(h > 0)
        def _():
            loop(0, per, lambda i: stage_in(0, (h - 1) * per + i))

    loop(0, chunks, last)
    loop(0, per, lambda i: stage_in(0, (chunks - 1) * per + i))
    stage_time(0)
    order = lambda i: lax.rem(F0 + i, RADIX)
    loop(0, RADIX, lambda i: stage_out(0, order(i)))

    def h_sent(f):
        for j in range(1, A):
            h_copy(j, f).wait_send()

    loop(0, RADIX, h_sent)

    def lends(f):
        return is_end & (f >= F0)

    def again(i):
        f = order(i)
        for j in range(1, A):
            g_copy_in(0, j, f).wait_recv()
        if lent:

            @pl.when(lends(f))
            def _():
                lend_g(f - F0).start()

            @pl.when(jnp.logical_not(lends(f)))
            def _():
                product(1, f)

            @pl.when(is_helper & (i >= 2) & (lax.rem(i, 2) == 0) & (i < 2 * Q + 2))
            def _():
                lent_product(1, i // 2 - 1)

            before = order(i + RADIX - 1)

            @pl.when((i > 0) & jnp.logical_not(lends(before)))
            def _():
                stage_in(1, before)

        else:
            product(1, f)

            @pl.when(i > 0)
            def _():
                stage_in(1, order(i + RADIX - 1))

    loop(0, RADIX, again)
    if lent:
        late = (RADIX - 1) // 2

        @pl.when(is_helper)
        def _():
            if late < Q:
                loop(late, Q, lambda n: lent_product(1, n))

        @pl.when(is_end)
        def _():
            loop(0, Q, returned)

    by_af[a] = squares[...]

    def af_copy(j):
        return remote(squares, by_af.at[a], m_send.at[j], m_recv.at[j], (ahead(j), s))

    def af_copy_in(j):
        return remote(squares, by_af.at[behind(j)], m_send.at[j], m_recv.at[j], (ahead(j), s))

    for j in range(1, A):
        af_copy(j).start()
    stage_in(1, order(RADIX - 1))
    if lent:

        @pl.when(is_end)
        def _():
            loop(0, Q, lambda n: stage_in(1, F0 + n))

    stage_time(1)
    for j in range(1, A):
        g_sent = lambda f: g_copy(0, j, f).wait_send()
        loop(0, RADIX, g_sent)
    loop(0, RADIX, lambda f: stage_out(1, f))

    for j in range(1, A):
        af_copy_in(j).wait_recv()
    total = by_af[0]
    for b in range(1, A):
        total = total + by_af[b]
    by_sa[s] = total
    for j in range(1, A):
        af_copy(j).wait_send()
    squares[...] = total

    def sa_copy(j):
        return remote(
            squares, by_sa.at[s], m_send.at[A + j], m_recv.at[A + j], (a, lax.rem(s + j, S))
        )

    def sa_copy_in(j):
        return remote(
            squares, by_sa.at[lax.rem(s + S - j, S)], m_send.at[A + j], m_recv.at[A + j], (a, lax.rem(s + j, S))
        )

    loop(1, S, lambda j: sa_copy(j).start())

    def sent(h):
        @pl.when(goes_up(h))
        def _():
            loop(0, c + 1, lambda chip: up(chip, h).wait_send())

        @pl.when(goes_down(h))
        def _():
            loop(c, C, lambda chip: down(chip, h).wait_send())

        @pl.when(keeps(h))
        def _():
            loop(0, C, lambda chip: across(chip, h).wait_send())

    loop(0, chunks, sent)
    if lent:

        @pl.when(is_helper)
        def _():
            loop(0, Q, lambda n: lend_h(n).wait_send())

    for j in range(1, A):
        for part in range(2):
            initials(part, j).wait_send()
    loop(0, RADIX, h_sent)
    loop(1, S, lambda j: sa_copy_in(j).wait_recv())
    full = by_sa[0]
    for b in range(1, S):
        full = full + by_sa[b]
    for it in range(ITERS):
        mis[it] = jnp.sum(full[it]) * (1.0 / (U * RADIX * A * N * N))
    loop(1, S, lambda j: sa_copy(j).wait_send())

    def finish(f):
        for j in range(1, A):
            g_copy_in(1, j, f).wait_recv()
            g_copy(1, j, f).wait_send()
        own_out(f).wait()

    loop(0, RADIX, finish)


def on_device(counts, data_real, data_imaginary, wave_real, wave_imaginary, primaries_real, primaries_imaginary):
    A, S = counts
    C = S // 2
    L, R, N = data_real.shape
    W = N // A
    U = L // RADIX
    chunks = RADIX if C <= 8 else 1
    lent = LENT if C >= 4 and chunks > LENT else 0
    Q = max(1, lent * RADIX // chunks)
    turns = 2 * np.pi * np.arange(RADIX * RADIX) / (RADIX * RADIX)
    twiddle = jnp.asarray(np.stack([np.cos(turns), np.sin(turns)]), jnp.float32)
    smem = pl.BlockSpec(memory_space=pltpu.SMEM)
    hbm = pl.BlockSpec(memory_space=pl.ANY)
    f32, bf16 = jnp.float32, jnp.bfloat16
    dma = pltpu.SemaphoreType.DMA
    split = lambda v: v.reshape(U, RADIX, R, N)
    coded, misfit = pl.pallas_call(
        functools.partial(kernel, A, S, chunks, lent),
        in_specs=[smem, smem, smem, hbm, hbm, hbm, hbm],
        out_specs=[hbm, smem],
        out_shape=[
            jax.ShapeDtypeStruct((2, U, RADIX, R, N), bf16),
            jax.ShapeDtypeStruct((ITERS,), f32),
        ],
        scratch_shapes=[
            pltpu.VMEM((U, RADIX, 2, S, R, N), bf16),
            pltpu.VMEM((2, U, RADIX, R, N), f32),
            pltpu.VMEM((2, A, U, RADIX, R, W), f32),
            pltpu.VMEM((2, RADIX, RADIX, R, W), f32),
            pltpu.VMEM((2, RADIX, RADIX, R, W), f32),
            pltpu.VMEM((A, 2, U, RADIX, R, W), bf16),
            pltpu.VMEM((A, 2, U, RADIX, R, W), bf16),
            pltpu.VMEM((A, 2, U, RADIX, R, W), bf16),
            pltpu.VMEM((2, U, RADIX, R, N), bf16),
            pltpu.VMEM((ITERS, 8, 128), f32),
            pltpu.VMEM((A, ITERS, 8, 128), f32),
            pltpu.VMEM((S, ITERS, 8, 128), f32),
            pltpu.VMEM((2, U, Q, R, N), bf16),
            pltpu.VMEM((A, 2, U, Q, R, W), bf16),
            dma((6,)),
            dma((C, chunks)),
            dma((C, chunks)),
            dma((C, chunks)),
            dma((C, chunks)),
            dma((C, chunks)),
            dma((2, A)),
            dma((2, A)),
            dma((A, RADIX)),
            dma((A, RADIX)),
            dma((ITERS, A, RADIX)),
            dma((ITERS, A, RADIX)),
            dma((A + S,)),
            dma((A + S,)),
            dma((Q,)),
            dma((Q,)),
            dma((Q,)),
            dma((Q,)),
            dma((RADIX,)),
        ],
        compiler_params=pltpu.CompilerParams(
            collective_id=0, has_side_effects=True, vmem_limit_bytes=63 * 2**20
        ),
    )(
        wave_real, wave_imaginary, twiddle,
        split(data_real), split(data_imaginary), split(primaries_real), split(primaries_imaginary),
    )
    updated = [decode(coded[part]).reshape(L, R, N) for part in range(2)]
    return (updated[0], updated[1], misfit)


def solution(mesh):
    split = P("af", "sa", None)
    counts = (mesh.shape["af"], mesh.shape["sa"])
    return jax.shard_map(
        functools.partial(on_device, counts),
        mesh=mesh,
        in_specs=(split, split, P("af"), P("af"), split, split),
        out_specs=(split, split, P()),
        check_vma=False,
    )
```

```python
import functools
import math

import jax
import jax.numpy as jnp
import numpy as np
from jax import lax
from jax.experimental import pallas as pl
from jax.experimental.pallas import tpu as pltpu
from jax.sharding import PartitionSpec as P

ITERS = 2
STEP_LENGTH = 0.02
THRESHOLD = 0.25
RADIX = 8
LENT = 3
LAG = 4
HALF = math.sqrt(0.5)
REACH = 64.0
TINY = 2.0**-126
MESH = pl.DeviceIdType.MESH


def encode(x):
    y = x * (1.0 / REACH)
    return ((y * y) * (y * jnp.abs(y))).astype(jnp.bfloat16)


def decode(code):
    v = code.astype(jnp.float32)
    y = lax.rsqrt(jnp.maximum(jnp.abs(v), TINY))
    return ((v * y) * y) * (lax.rsqrt(y) * REACH)


def add(a, b):
    return (a[0] + b[0], a[1] + b[1])


def sub(a, b):
    return (a[0] - b[0], a[1] - b[1])


def turn(a, sign):
    return (-a[1], a[0]) if sign > 0 else (a[1], -a[0])


def rotate(a, c, s):
    return (a[0] * c - a[1] * s, a[0] * s + a[1] * c)


def four(a, b, c, d, sign):
    s0, s1, s2, s3 = add(a, c), sub(a, c), add(b, d), turn(sub(b, d), sign)
    return add(s0, s2), add(s1, s3), sub(s0, s2), sub(s1, s3)


def eight(x, sign):
    even = four(x[0], x[2], x[4], x[6], sign)
    odd = four(x[1], x[3], x[5], x[7], sign)
    o1 = add(odd[1], turn(odd[1], sign))
    o3 = sub(turn(odd[3], sign), odd[3])
    odd = (odd[0], (o1[0] * HALF, o1[1] * HALF), turn(odd[2], sign), (o3[0] * HALF, o3[1] * HALF))
    return [add(even[k], odd[k]) for k in range(4)] + [sub(even[k], odd[k]) for k in range(4)]


def shrink(v):
    return v - jnp.clip(v, -THRESHOLD, THRESHOLD)


def loop(start, stop, body):
    def step(i, _):
        body(i)
        return 0

    lax.fori_loop(start, stop, step, 0)


def kernel(
    A, S, chunks, F0, wr, wi, twiddle, data_r, data_i, prim_r, prim_i, out_r, out_i, mis,
    whole, current, initial, work, traces, hs, hr, gs, gr, squares, by_af, by_sa, lent_g, lent_h,
    local_sem, up_sem, down_sem, ring_sem, pair_send, pair_recv,
    init_send, init_recv, h_send, h_recv, g_send, g_recv, o_send, o_recv, m_send, m_recv,
    lg_send, lg_recv, lh_send, lh_recv, out_sem,
):
    C = S // 2
    L, R, N = prim_r.shape
    U = L // RADIX
    W = N // A
    per = RADIX // chunks
    halves = 2 if R % 32 == 0 else 1
    half = R // halves
    rows = 16 if R % 16 == 0 else 8
    a = lax.axis_index("af")
    s = lax.axis_index("sa")
    c = s // 2
    k = s % 2
    partner = c * 2 + 1 - k
    kept = F0 // per
    lent = chunks - kept
    Q = L - F0 * U
    if lent:
        is_end = (c == 0) | (c == C - 1)
        is_helper = (c == 1) | (c == C - 2)
        other = jnp.where((c == 0) | (c == C - 2), s + 2, s - 2)

    def goes_up(h):
        go = c + 1 < C
        return go & ((h < kept) | (c + 2 < C)) if lent else go

    def goes_down(h):
        go = c > 0
        return go & ((h < kept) | (c > 1)) if lent else go

    def keeps(h):
        return (h < kept) | jnp.logical_not(is_end) if lent else h >= 0

    mine = pl.ds(pl.multiple_of(a * W, W), W)

    def place(n):
        return lax.rem(n, U) * RADIX + n // U

    def cols(b):
        return pl.ds(pl.multiple_of(b * W, W), W)

    def ahead(j):
        return lax.rem(a + j, A)

    def behind(j):
        return lax.rem(a + A - j, A)

    barrier = pltpu.get_barrier_semaphore()
    for j in range(1, A):
        pl.semaphore_signal(barrier, inc=1, device_id=(ahead(j), s), device_id_type=MESH)
    loop(
        1, S,
        lambda j: pl.semaphore_signal(barrier, inc=1, device_id=(a, lax.rem(s + j, S)), device_id_type=MESH),
    )

    locals_ = [
        pltpu.make_async_copy(data_r, whole.at[:, :, 0, s], local_sem.at[0]),
        pltpu.make_async_copy(data_i, whole.at[:, :, 1, s], local_sem.at[1]),
        pltpu.make_async_copy(prim_r, current.at[0], local_sem.at[2]),
        pltpu.make_async_copy(prim_i, current.at[1], local_sem.at[3]),
        pltpu.make_async_copy(prim_r.at[:, :, mine], initial.at[0, a], local_sem.at[4]),
        pltpu.make_async_copy(prim_i.at[:, :, mine], initial.at[1, a], local_sem.at[5]),
    ]
    for copy in locals_:
        copy.start()
    squares[...] = jnp.zeros_like(squares)
    pl.semaphore_wait(barrier, A - 1 + S - 1)

    def shard(chip, core, h):
        return whole.at[:, pl.ds(h * per, per), :, chip * 2 + core]

    def remote(src, dst, send, recv, device):
        return pltpu.make_async_remote_copy(
            src_ref=src, dst_ref=dst, send_sem=send, recv_sem=recv, device_id=device, device_id_type=MESH
        )

    def own(part, h):
        return (data_r, data_i)[part].at[:, pl.ds(h * per, per)]

    def up(chip, h):
        ref = shard(chip, k, h)
        return remote(ref, ref, up_sem.at[chip, h], ring_sem.at[chip, h], (a, lax.rem(s + 2, S)))

    def down(chip, h):
        ref = shard(chip, k, h)
        return remote(ref, ref, down_sem.at[chip, h], ring_sem.at[chip, h], (a, lax.rem(s + S - 2, S)))

    def across(chip, h):
        ref = shard(chip, k, h)
        return remote(ref, ref, pair_send.at[chip, h], pair_recv.at[chip, h], (a, partner))

    def own_up(part, h):
        return remote(
            own(part, h), shard(c, k, h).at[:, :, part], up_sem.at[c, h], ring_sem.at[c, h], (a, lax.rem(s + 2, S))
        )

    def own_down(part, h):
        return remote(
            own(part, h), shard(c, k, h).at[:, :, part], down_sem.at[c, h], ring_sem.at[c, h], (a, lax.rem(s + S - 2, S))
        )

    def own_across(part, h):
        return remote(
            own(part, h), shard(c, k, h).at[:, :, part], pair_send.at[c, h], pair_recv.at[c, h], (a, partner)
        )

    def across_in(chip, h):
        ref = shard(chip, 1 - k, h)
        return remote(ref, ref, pair_send.at[chip, h], pair_recv.at[chip, h], (a, partner))

    def initials(part, j):
        src = (prim_r, prim_i)[part]
        return remote(
            src.at[:, :, cols(ahead(j))], initial.at[part, a],
            init_send.at[part, j], init_recv.at[part, j], (ahead(j), s),
        )

    def initials_in(part, j):
        src = (prim_r, prim_i)[part]
        return remote(
            src.at[:, :, mine], initial.at[part, behind(j)],
            init_send.at[part, j], init_recv.at[part, j], (ahead(j), s),
        )

    def first(h):
        @pl.when(goes_up(h))
        def _():
            own_up(0, h).start()
            own_up(1, h).start()

        @pl.when(goes_down(h))
        def _():
            own_down(0, h).start()
            own_down(1, h).start()

        @pl.when(keeps(h))
        def _():
            own_across(0, h).start()
            own_across(1, h).start()

    loop(0, chunks, first)

    def lend_g(n):
        return remote(gr.at[:, lax.rem(n, U), F0 + n // U], lent_g.at[:, n], lg_send.at[n], lg_recv.at[n], (a, other))

    def lend_h(n):
        return remote(lent_h.at[:, :, n], hs.at[:, :, lax.rem(n, U), F0 + n // U], lh_send.at[n], lh_recv.at[n], (a, other))

    for j in range(1, A):
        for part in range(2):
            initials(part, j).start()
    for copy in locals_[2:4]:
        copy.wait()
    if lent:

        @pl.when(is_end)
        def _():
            def lend(n):
                at = place(F0 * U + n)
                for part in range(2):
                    gr[part, lax.rem(n, U), F0 + n // U] = current[part, at].astype(jnp.bfloat16)
                lend_g(n).start()

            loop(0, Q, lend)


    def arrive(d, h):
        @pl.when(c >= d)
        def _():
            src = c - d
            up(src, h).wait_recv()
            across(src, h).start()

            @pl.when(goes_up(h))
            def _():
                up(src, h).start()

        @pl.when(c + d < C)
        def _():
            src = c + d
            down(src, h).wait_recv()
            across(src, h).start()

            @pl.when(goes_down(h))
            def _():
                down(src, h).start()

    far = jnp.maximum(c, C - 1 - c)

    def pass_on(h, d):
        @pl.when(keeps(h))
        def _():
            arrive(d, h)

    loop(1, far, lambda d: loop(0, chunks, lambda h: pass_on(h, d)))

    def strip(p):
        return pl.ds(pl.multiple_of(p * half, half), half)

    def h_copy(j, f, p):
        to, q, at = ahead(j), f * halves + p, strip(p)
        return remote(hs.at[to, :, :, f, at], hr.at[a, :, :, f, at], h_send.at[j, q], h_recv.at[j, q], (to, s))

    def h_copy_in(j, f, p):
        q, at = f * halves + p, strip(p)
        return remote(
            hs.at[a, :, :, f, at], hr.at[behind(j), :, :, f, at], h_send.at[j, q], h_recv.at[j, q], (ahead(j), s)
        )

    def g_copy(j, f):
        to = ahead(j)
        return remote(gs.at[to, :, :, f], gr.at[:, :, f, :, mine], g_send.at[j, f], g_recv.at[j, f], (to, s))

    def g_copy_in(j, f):
        return remote(
            gs.at[a, :, :, f], gr.at[:, :, f, :, cols(behind(j))], g_send.at[j, f], g_recv.at[j, f], (ahead(j), s)
        )

    def o_copy(part, j, m, p):
        to, q, at, pair = ahead(j), m * halves + p, strip(p), pl.ds(m * 2, 2)
        return remote(
            gs.at[to, part, :, pair, at], (out_r, out_i)[part].at[:, pair, at, mine],
            o_send.at[j, q], o_recv.at[j, q], (to, s),
        )

    def o_both(j, m, p):
        q, at, pair = m * halves + p, strip(p), pl.ds(m * 2, 2)
        return remote(
            gs.at[a, :, :, pair, at], gr.at[:, :, pair, at, cols(behind(j))],
            o_send.at[j, q], o_recv.at[j, q], (ahead(j), s),
        )

    def step_of(it, l, at, re, im):
        u, f = l // RADIX, lax.rem(l, RADIX)
        qr = wr[l]
        qi = wi[l]
        whole_r = whole[u, f, 0].reshape(N, N)
        whole_i = whole[u, f, 1].reshape(N, N)
        left = jnp.concatenate([re.astype(jnp.bfloat16), im.astype(jnp.bfloat16)], axis=0)
        pr = jnp.dot(left, whole_r, preferred_element_type=jnp.float32)
        pi = jnp.dot(left, whole_i, preferred_element_type=jnp.float32)
        er = whole[u, f, 0, at].astype(jnp.float32) + (pr[:R] - pi[R:]) - (qr * re - qi * im)
        ei = whole[u, f, 1, at].astype(jnp.float32) + (pi[:R] + pr[R:]) - (qr * im + qi * re)
        sq = er * er + ei * ei
        part = sq[:8]
        for i in range(1, R // 8):
            part = part + sq[i * 8 : (i + 1) * 8]
        row = part[:, :128]
        for i in range(1, N // 128):
            row = row + part[:, i * 128 : (i + 1) * 128]
        squares[it] += row
        eb = jnp.concatenate([er.astype(jnp.bfloat16), ei.astype(jnp.bfloat16)], axis=0)
        dims = (((1,), (1,)), ((), ()))
        br = lax.dot_general(eb, whole_r, dims, preferred_element_type=jnp.float32)
        bi = lax.dot_general(eb, whole_i, dims, preferred_element_type=jnp.float32)
        dr = encode(STEP_LENGTH * (qr * er + qi * ei - (br[:R] + bi[R:])))
        di = encode(STEP_LENGTH * (qr * ei - qi * er - (br[R:] - bi[:R])))
        return dr, di

    def publish(it, l):
        u, f = l // RADIX, lax.rem(l, RADIX)
        hr[a, 0, u, f] = hs[a, 0, u, f]
        hr[a, 1, u, f] = hs[a, 1, u, f]

        @pl.when(u == U - 1)
        def _():
            for p in range(halves if it == 0 else 1):
                for j in range(1, A):
                    h_copy(j, f, p).start()

    def product(it, l):
        u, f = l // RADIX, lax.rem(l, RADIX)
        if it == 0:
            re, im = current[0, l], current[1, l]
        else:
            re, im = gr[0, u, f].astype(jnp.float32), gr[1, u, f].astype(jnp.float32)
        dr, di = step_of(it, l, s, re, im)
        for b in range(A):
            hs[b, 0, u, f] = dr[:, b * W : (b + 1) * W]
            hs[b, 1, u, f] = di[:, b * W : (b + 1) * W]
        publish(it, l)

    def lent_product(it, n):
        lend_g(n).wait_recv()
        if it > 0:
            lend_h(n).wait_send()
        dr, di = step_of(
            it, place(F0 * U + n), other, lent_g[0, n].astype(jnp.float32), lent_g[1, n].astype(jnp.float32)
        )
        for b in range(A):
            lent_h[b, 0, n] = dr[:, b * W : (b + 1) * W]
            lent_h[b, 1, n] = di[:, b * W : (b + 1) * W]
        lend_h(n).start()

    def returned(it, n):
        lend_h(n).wait_recv()
        lend_g(n).wait_send()
        publish(it, place(F0 * U + n))

    blocks = half // rows

    def stage_in(it, f, p):
        for j in range(1, A):
            h_copy_in(j, f, p).wait_recv()

        def some(g):
            at = pl.ds(pl.multiple_of(g * rows, rows), rows)
            x = []
            for f2 in range(RADIX):
                b, u = divmod(f2, U)
                l = u * RADIX + f
                re = decode(hr[b, 0, u, f, at, :])
                im = decode(hr[b, 1, u, f, at, :])
                if it == 0:
                    re = re + initial[0, b, l, at, :]
                    im = im + initial[1, b, l, at, :]
                x.append((re * (1.0 / RADIX), im * (1.0 / RADIX)))
            y = eight(x, 1)
            for t in range(RADIX):
                v = rotate(y[t], twiddle[0, f * t], twiddle[1, f * t]) if t else y[t]
                work[0, f, t, at, :] = v[0]
                work[1, f, t, at, :] = v[1]

        loop(p * blocks, p * blocks + blocks, some)

    def stage_time(it, p):
        def some(g):
            at = pl.ds(pl.multiple_of(g * rows, rows), rows)

            def one(t):
                y = eight([(work[0, f, t, at, :], work[1, f, t, at, :]) for f in range(RADIX)], 1)
                if it > 0:
                    y = [(v[0] + traces[0, n, t, at, :], v[1] + traces[1, n, t, at, :]) for n, v in enumerate(y)]
                y = [(shrink(v[0]), shrink(v[1])) for v in y]
                if it < ITERS - 1:
                    for n, v in enumerate(y):
                        traces[0, n, t, at, :] = v[0]
                        traces[1, n, t, at, :] = v[1]
                y = eight(y, -1)
                for f in range(RADIX):
                    v = rotate(y[f], twiddle[0, f * t], -twiddle[1, f * t]) if f else y[f]
                    work[0, f, t, at, :] = v[0]
                    work[1, f, t, at, :] = v[1]

            loop(0, RADIX, one)

        loop(p * blocks, p * blocks + blocks, some)

    def own_out(part, m, p):
        at, pair = strip(p), pl.ds(m * 2, 2)
        return pltpu.make_async_copy(
            gs.at[a, part, :, pair, at], (out_r, out_i)[part].at[:, pair, at, mine], out_sem.at[part, m * halves + p]
        )

    def stage_out(it, f, p):
        def some(g):
            at = pl.ds(pl.multiple_of(g * rows, rows), rows)
            y = eight([(work[0, f, t, at, :], work[1, f, t, at, :]) for t in range(RADIX)], -1)
            for f2 in range(RADIX):
                b, u = divmod(f2, U)
                for part in range(2):
                    v = y[f2][part] * (1.0 / RADIX)
                    gs[b, part, u, f, at, :] = v.astype(jnp.bfloat16) if it == 0 else encode(v)

        loop(p * blocks, p * blocks + blocks, some)

    def give_back(f):
        for p in range(halves):
            stage_out(0, f, p)
        for j in range(1, A):
            g_copy(j, f).start()
        for part in range(2):
            for u in range(U):
                gr[part, u, f, :, mine] = gs[a, part, u, f]

    def give_out(m, p):
        stage_out(1, 2 * m, p)
        stage_out(1, 2 * m + 1, p)
        for j in range(1, A):
            o_copy(0, j, m, p).start()
            o_copy(1, j, m, p).start()
        for part in range(2):
            own_out(part, m, p).start()

    for copy in locals_[:2] + locals_[4:]:
        copy.wait()
    for j in range(1, A):
        for part in range(2):
            initials_in(part, j).wait_recv()

    def last(h):
        @pl.when(keeps(h))
        def _():
            arrive(far, h)
            loop(0, C, lambda chip: across_in(chip, h).wait_recv())

        def slot(i):
            n = h * per * U + i
            if lent:

                @pl.when(is_helper & (n >= F0 * U))
                def _():
                    lent_product(0, n - F0 * U)

                @pl.when(is_end & (n >= F0 * U))
                def _():
                    returned(0, n - F0 * U)

            @pl.when(keeps(h))
            def _():
                product(0, place(n))

            @pl.when((n >= U) & (lax.rem(n, U) == U - 1))
            def _():
                for p in range(halves):
                    stage_in(0, n // U - 1, p)

        loop(0, per * U, slot)

    loop(0, chunks, last)
    for p in range(halves):
        stage_in(0, RADIX - 1, p)
    order = lambda i: lax.rem(F0 + i, RADIX)

    loop(0, halves, lambda p: stage_time(0, p))
    loop(0, RADIX, lambda i: give_back(order(i)))

    def h_sent(f):
        for p in range(halves):
            for j in range(1, A):
                h_copy(j, f, p).wait_send()

    loop(0, RADIX, h_sent)

    def again(i):
        n = lax.rem(F0 * U + i, L)
        l = place(n)

        @pl.when(lax.rem(n, U) == 0)
        def _():
            for j in range(1, A):
                g_copy_in(j, n // U).wait_recv()

        if lent:
            lends = is_end & (n >= F0 * U)

            @pl.when(lends)
            def _():
                lend_g(n - F0 * U).start()

            @pl.when(jnp.logical_not(lends))
            def _():
                product(1, l)

            @pl.when(is_helper & (i >= LAG) & (lax.rem(i, 2) == 0) & (i < 2 * Q + LAG))
            def _():
                lent_product(1, (i - LAG) // 2)

        else:
            product(1, l)

    loop(0, L, again)
    if lent:
        late = (L - LAG + 1) // 2

        @pl.when(is_helper)
        def _():
            if late < Q:
                loop(late, Q, lambda n: lent_product(1, n))

        @pl.when(is_end)
        def _():
            loop(0, Q, lambda n: returned(1, n))


    def rest(f):
        for p in range(1, halves):
            for j in range(1, A):
                h_copy(j, f, p).start()

    loop(0, RADIX, rest)
    by_af[a] = squares[...]

    def af_copy(j):
        return remote(squares, by_af.at[a], m_send.at[j], m_recv.at[j], (ahead(j), s))

    def af_copy_in(j):
        return remote(squares, by_af.at[behind(j)], m_send.at[j], m_recv.at[j], (ahead(j), s))

    for j in range(1, A):
        af_copy(j).start()

    def g_sent(f):
        for j in range(1, A):
            g_copy(j, f).wait_send()

    loop(0, RADIX, g_sent)

    def turn_over(p):
        loop(0, RADIX, lambda i: stage_in(1, order(i + RADIX - F0), p))
        stage_time(1, p)
        loop(0, RADIX // 2, lambda m: give_out(m, p))

    loop(0, halves, turn_over)

    for j in range(1, A):
        af_copy_in(j).wait_recv()
    total = by_af[0]
    for b in range(1, A):
        total = total + by_af[b]
    by_sa[s] = total
    for j in range(1, A):
        af_copy(j).wait_send()
    squares[...] = total

    def sa_copy(j):
        return remote(
            squares, by_sa.at[s], m_send.at[A + j], m_recv.at[A + j], (a, lax.rem(s + j, S))
        )

    def sa_copy_in(j):
        return remote(
            squares, by_sa.at[lax.rem(s + S - j, S)], m_send.at[A + j], m_recv.at[A + j], (a, lax.rem(s + j, S))
        )

    loop(1, S, lambda j: sa_copy(j).start())

    def sent(h):
        @pl.when(goes_up(h))
        def _():
            loop(0, c + 1, lambda chip: up(chip, h).wait_send())

        @pl.when(goes_down(h))
        def _():
            loop(c, C, lambda chip: down(chip, h).wait_send())

        @pl.when(keeps(h))
        def _():
            loop(0, C, lambda chip: across(chip, h).wait_send())

    loop(0, chunks, sent)
    if lent:

        @pl.when(is_helper)
        def _():
            loop(0, Q, lambda n: lend_h(n).wait_send())

    for j in range(1, A):
        for part in range(2):
            initials(part, j).wait_send()
    loop(0, RADIX, h_sent)
    loop(1, S, lambda j: sa_copy_in(j).wait_recv())
    full = by_sa[0]
    for b in range(1, S):
        full = full + by_sa[b]
    for it in range(ITERS):
        mis[it] = jnp.sum(full[it]) * (1.0 / (U * RADIX * A * N * N))
    loop(1, S, lambda j: sa_copy(j).wait_send())

    def finish(m):
        for p in range(halves):
            for j in range(1, A):
                o_both(j, m, p).wait_recv()
                o_both(j, m, p).wait_send()
            for part in range(2):
                own_out(part, m, p).wait()

    loop(0, RADIX // 2, finish)


def on_device(counts, data_real, data_imaginary, wave_real, wave_imaginary, primaries_real, primaries_imaginary):
    A, S = counts
    C = S // 2
    L, R, N = data_real.shape
    W = N // A
    U = L // RADIX
    chunks = RADIX if C <= 8 else 1
    halves = 2 if R % 32 == 0 else 1
    split = lambda v: v.reshape(U, RADIX, R, N)
    kept = RADIX - LENT if C >= 4 and chunks > 1 else RADIX
    Q = max(1, (RADIX - kept) * U)
    turns = 2 * np.pi * np.arange(RADIX * RADIX) / (RADIX * RADIX)
    twiddle = jnp.asarray(np.stack([np.cos(turns), np.sin(turns)]), jnp.float32)
    smem = pl.BlockSpec(memory_space=pltpu.SMEM)
    hbm = pl.BlockSpec(memory_space=pl.ANY)
    f32, bf16 = jnp.float32, jnp.bfloat16
    dma = pltpu.SemaphoreType.DMA
    coded_r, coded_i, misfit = pl.pallas_call(
        functools.partial(kernel, A, S, chunks, kept),
        in_specs=[smem, smem, smem, hbm, hbm, hbm, hbm],
        out_specs=[hbm, hbm, smem],
        out_shape=[
            jax.ShapeDtypeStruct((U, RADIX, R, N), bf16),
            jax.ShapeDtypeStruct((U, RADIX, R, N), bf16),
            jax.ShapeDtypeStruct((ITERS,), f32),
        ],
        scratch_shapes=[
            pltpu.VMEM((U, RADIX, 2, S, R, N), bf16),
            pltpu.VMEM((2, L, R, N), f32),
            pltpu.VMEM((2, A, L, R, W), f32),
            pltpu.VMEM((2, RADIX, RADIX, R, W), f32),
            pltpu.VMEM((2, RADIX, RADIX, R, W), f32),
            pltpu.VMEM((A, 2, U, RADIX, R, W), bf16),
            pltpu.VMEM((A, 2, U, RADIX, R, W), bf16),
            pltpu.VMEM((A, 2, U, RADIX, R, W), bf16),
            pltpu.VMEM((2, U, RADIX, R, N), bf16),
            pltpu.VMEM((ITERS, 8, 128), f32),
            pltpu.VMEM((A, ITERS, 8, 128), f32),
            pltpu.VMEM((S, ITERS, 8, 128), f32),
            pltpu.VMEM((2, Q, R, N), bf16),
            pltpu.VMEM((A, 2, Q, R, W), bf16),
            dma((6,)),
            dma((C, chunks)),
            dma((C, chunks)),
            dma((C, chunks)),
            dma((C, chunks)),
            dma((C, chunks)),
            dma((2, A)),
            dma((2, A)),
            dma((A, RADIX * halves)),
            dma((A, RADIX * halves)),
            dma((A, RADIX)),
            dma((A, RADIX)),
            dma((A, RADIX * halves // 2)),
            dma((A, RADIX * halves // 2)),
            dma((A + S,)),
            dma((A + S,)),
            dma((Q,)),
            dma((Q,)),
            dma((Q,)),
            dma((Q,)),
            dma((2, RADIX * halves // 2)),
        ],
        compiler_params=pltpu.CompilerParams(
            collective_id=0, has_side_effects=True, vmem_limit_bytes=63 * 2**20
        ),
    )(
        wave_real, wave_imaginary, twiddle,
        split(data_real), split(data_imaginary), primaries_real, primaries_imaginary,
    )
    return (decode(coded_r).reshape(L, R, N), decode(coded_i).reshape(L, R, N), misfit)


def solution(mesh):
    split = P("af", "sa", None)
    counts = (mesh.shape["af"], mesh.shape["sa"])
    return jax.shard_map(
        functools.partial(on_device, counts),
        mesh=mesh,
        in_specs=(split, split, P("af"), P("af"), split, split),
        out_specs=(split, split, P()),
        check_vma=False,
    )
```

```python
import functools
import math

import jax
import jax.numpy as jnp
import numpy as np
from jax import lax
from jax.experimental import pallas as pl
from jax.experimental.pallas import tpu as pltpu
from jax.sharding import PartitionSpec as P

ITERS = 2
STEP_LENGTH = 0.02
THRESHOLD = 0.25
RADIX = 8
LENT = 3
LAG = 4
HALF = math.sqrt(0.5)
REACH = 64.0
TINY = 2.0**-126
MESH = pl.DeviceIdType.MESH


def encode(x):
    y = x * (1.0 / REACH)
    return ((y * y) * (y * jnp.abs(y))).astype(jnp.bfloat16)


def decode(code):
    v = code.astype(jnp.float32)
    y = lax.rsqrt(jnp.maximum(jnp.abs(v), TINY))
    return ((v * y) * y) * (lax.rsqrt(y) * REACH)


def add(a, b):
    return (a[0] + b[0], a[1] + b[1])


def sub(a, b):
    return (a[0] - b[0], a[1] - b[1])


def turn(a, sign):
    return (-a[1], a[0]) if sign > 0 else (a[1], -a[0])


def rotate(a, c, s):
    return (a[0] * c - a[1] * s, a[0] * s + a[1] * c)


def four(a, b, c, d, sign):
    s0, s1, s2, s3 = add(a, c), sub(a, c), add(b, d), turn(sub(b, d), sign)
    return add(s0, s2), add(s1, s3), sub(s0, s2), sub(s1, s3)


def eight(x, sign):
    even = four(x[0], x[2], x[4], x[6], sign)
    odd = four(x[1], x[3], x[5], x[7], sign)
    o1 = add(odd[1], turn(odd[1], sign))
    o3 = sub(turn(odd[3], sign), odd[3])
    odd = (odd[0], (o1[0] * HALF, o1[1] * HALF), turn(odd[2], sign), (o3[0] * HALF, o3[1] * HALF))
    return [add(even[k], odd[k]) for k in range(4)] + [sub(even[k], odd[k]) for k in range(4)]


def shrink(v):
    return v - jnp.clip(v, -THRESHOLD, THRESHOLD)


def loop(start, stop, body):
    def step(i, _):
        body(i)
        return 0

    lax.fori_loop(start, stop, step, 0)


def kernel(
    A, S, chunks, F0, wr, wi, twiddle, data_r, data_i, prim_r, prim_i, out_r, out_i, mis,
    whole, current, initial, work, traces, hs, hr, gs, gr, squares, by_af, by_sa, lent_g, lent_h,
    local_sem, up_sem, down_sem, ring_sem, pair_send, pair_recv,
    init_send, init_recv, h_send, h_recv, g_send, g_recv, o_send, o_recv, m_send, m_recv,
    lg_send, lg_recv, lh_send, lh_recv, out_sem,
):
    C = S // 2
    L, R, N = prim_r.shape
    U = L // RADIX
    W = N // A
    per = RADIX // chunks
    halves = 2 if R % 32 == 0 else 1
    half = R // halves
    rows = 16 if R % 16 == 0 else 8
    a = lax.axis_index("af")
    s = lax.axis_index("sa")
    c = s // 2
    k = s % 2
    partner = c * 2 + 1 - k
    kept = F0 // per
    lent = chunks - kept
    Q = L - F0 * U
    if lent:
        is_end = (c == 0) | (c == C - 1)
        is_helper = (c == 1) | (c == C - 2)
        other = jnp.where((c == 0) | (c == C - 2), s + 2, s - 2)

    def goes_up(h):
        go = c + 1 < C
        return go & ((h < kept) | (c + 2 < C)) if lent else go

    def goes_down(h):
        go = c > 0
        return go & ((h < kept) | (c > 1)) if lent else go

    def keeps(h):
        return (h < kept) | jnp.logical_not(is_end) if lent else h >= 0

    mine = pl.ds(pl.multiple_of(a * W, W), W)

    def place(n):
        return lax.rem(n, U) * RADIX + n // U

    def cols(b):
        return pl.ds(pl.multiple_of(b * W, W), W)

    def ahead(j):
        return lax.rem(a + j, A)

    def behind(j):
        return lax.rem(a + A - j, A)

    barrier = pltpu.get_barrier_semaphore()
    for j in range(1, A):
        pl.semaphore_signal(barrier, inc=1, device_id=(ahead(j), s), device_id_type=MESH)
    loop(
        1, S,
        lambda j: pl.semaphore_signal(barrier, inc=1, device_id=(a, lax.rem(s + j, S)), device_id_type=MESH),
    )

    locals_ = [
        pltpu.make_async_copy(data_r, whole.at[:, :, 0, s], local_sem.at[0]),
        pltpu.make_async_copy(data_i, whole.at[:, :, 1, s], local_sem.at[1]),
        pltpu.make_async_copy(prim_r, current.at[0], local_sem.at[2]),
        pltpu.make_async_copy(prim_i, current.at[1], local_sem.at[3]),
        pltpu.make_async_copy(prim_r.at[:, :, mine], initial.at[0, a], local_sem.at[4]),
        pltpu.make_async_copy(prim_i.at[:, :, mine], initial.at[1, a], local_sem.at[5]),
    ]
    for copy in locals_:
        copy.start()
    squares[...] = jnp.zeros_like(squares)
    pl.semaphore_wait(barrier, A - 1 + S - 1)

    def shard(chip, core, h):
        return whole.at[:, pl.ds(h * per, per), :, chip * 2 + core]

    def remote(src, dst, send, recv, device):
        return pltpu.make_async_remote_copy(
            src_ref=src, dst_ref=dst, send_sem=send, recv_sem=recv, device_id=device, device_id_type=MESH
        )

    def own(part, h):
        return (data_r, data_i)[part].at[:, pl.ds(h * per, per)]

    def up(chip, h):
        ref = shard(chip, k, h)
        return remote(ref, ref, up_sem.at[chip, h], ring_sem.at[chip, h], (a, lax.rem(s + 2, S)))

    def down(chip, h):
        ref = shard(chip, k, h)
        return remote(ref, ref, down_sem.at[chip, h], ring_sem.at[chip, h], (a, lax.rem(s + S - 2, S)))

    def across(chip, h):
        ref = shard(chip, k, h)
        return remote(ref, ref, pair_send.at[chip, h], pair_recv.at[chip, h], (a, partner))

    def own_up(part, h):
        return remote(
            own(part, h), shard(c, k, h).at[:, :, part], up_sem.at[c, h], ring_sem.at[c, h], (a, lax.rem(s + 2, S))
        )

    def own_down(part, h):
        return remote(
            own(part, h), shard(c, k, h).at[:, :, part], down_sem.at[c, h], ring_sem.at[c, h], (a, lax.rem(s + S - 2, S))
        )

    def own_across(part, h):
        return remote(
            own(part, h), shard(c, k, h).at[:, :, part], pair_send.at[c, h], pair_recv.at[c, h], (a, partner)
        )

    def across_in(chip, h):
        ref = shard(chip, 1 - k, h)
        return remote(ref, ref, pair_send.at[chip, h], pair_recv.at[chip, h], (a, partner))

    def initials(part, j):
        src = (prim_r, prim_i)[part]
        return remote(
            src.at[:, :, cols(ahead(j))], initial.at[part, a],
            init_send.at[part, j], init_recv.at[part, j], (ahead(j), s),
        )

    def initials_in(part, j):
        src = (prim_r, prim_i)[part]
        return remote(
            src.at[:, :, mine], initial.at[part, behind(j)],
            init_send.at[part, j], init_recv.at[part, j], (ahead(j), s),
        )

    def first(h):
        @pl.when(goes_up(h))
        def _():
            own_up(0, h).start()
            own_up(1, h).start()

        @pl.when(goes_down(h))
        def _():
            own_down(0, h).start()
            own_down(1, h).start()

        @pl.when(keeps(h))
        def _():
            own_across(0, h).start()
            own_across(1, h).start()

    loop(0, chunks, first)

    def lend_g(n):
        return remote(gr.at[:, lax.rem(n, U), F0 + n // U], lent_g.at[:, n], lg_send.at[n], lg_recv.at[n], (a, other))

    def lend_h(n):
        return remote(lent_h.at[:, :, n], hs.at[:, :, lax.rem(n, U), F0 + n // U], lh_send.at[n], lh_recv.at[n], (a, other))

    for j in range(1, A):
        for part in range(2):
            initials(part, j).start()
    for copy in locals_[2:4]:
        copy.wait()
    if lent:

        @pl.when(is_end)
        def _():
            def lend(n):
                at = place(F0 * U + n)
                for part in range(2):
                    gr[part, lax.rem(n, U), F0 + n // U] = current[part, at].astype(jnp.bfloat16)
                lend_g(n).start()

            loop(0, Q, lend)


    def arrive(d, h):
        @pl.when(c >= d)
        def _():
            src = c - d
            up(src, h).wait_recv()
            across(src, h).start()

            @pl.when(goes_up(h))
            def _():
                up(src, h).start()

        @pl.when(c + d < C)
        def _():
            src = c + d
            down(src, h).wait_recv()
            across(src, h).start()

            @pl.when(goes_down(h))
            def _():
                down(src, h).start()

    far = jnp.maximum(c, C - 1 - c)

    def pass_on(h, d):
        @pl.when(keeps(h))
        def _():
            arrive(d, h)

    loop(1, far, lambda d: loop(0, chunks, lambda h: pass_on(h, d)))

    def strip(p):
        return pl.ds(pl.multiple_of(p * half, half), half)

    def h_copy(j, f, p):
        to, q, at = ahead(j), f * halves + p, strip(p)
        return remote(hs.at[to, :, :, f, at], hr.at[a, :, :, f, at], h_send.at[j, q], h_recv.at[j, q], (to, s))

    def h_copy_in(j, f, p):
        q, at = f * halves + p, strip(p)
        return remote(
            hs.at[a, :, :, f, at], hr.at[behind(j), :, :, f, at], h_send.at[j, q], h_recv.at[j, q], (ahead(j), s)
        )

    def g_copy(j, f):
        to = ahead(j)
        return remote(gs.at[to, :, :, f], gr.at[:, :, f, :, mine], g_send.at[j, f], g_recv.at[j, f], (to, s))

    def g_copy_in(j, f):
        return remote(
            gs.at[a, :, :, f], gr.at[:, :, f, :, cols(behind(j))], g_send.at[j, f], g_recv.at[j, f], (ahead(j), s)
        )

    def o_copy(part, j, m, p):
        to, q, at, pair = ahead(j), m * halves + p, strip(p), pl.ds(m * 2, 2)
        return remote(
            gs.at[to, part, :, pair, at], (out_r, out_i)[part].at[:, pair, at, mine],
            o_send.at[j, q], o_recv.at[j, q], (to, s),
        )

    def o_both(j, m, p):
        q, at, pair = m * halves + p, strip(p), pl.ds(m * 2, 2)
        return remote(
            gs.at[a, :, :, pair, at], gr.at[:, :, pair, at, cols(behind(j))],
            o_send.at[j, q], o_recv.at[j, q], (ahead(j), s),
        )

    def step_of(it, l, at, re, im):
        u, f = l // RADIX, lax.rem(l, RADIX)
        qr = wr[l]
        qi = wi[l]
        whole_r = whole[u, f, 0].reshape(N, N)
        whole_i = whole[u, f, 1].reshape(N, N)
        left = jnp.concatenate([re.astype(jnp.bfloat16), im.astype(jnp.bfloat16)], axis=0)
        pr = jnp.dot(left, whole_r, preferred_element_type=jnp.float32)
        pi = jnp.dot(left, whole_i, preferred_element_type=jnp.float32)
        er = whole[u, f, 0, at].astype(jnp.float32) + (pr[:R] - pi[R:]) - (qr * re - qi * im)
        ei = whole[u, f, 1, at].astype(jnp.float32) + (pi[:R] + pr[R:]) - (qr * im + qi * re)
        sq = er * er + ei * ei
        part = sq[:8]
        for i in range(1, R // 8):
            part = part + sq[i * 8 : (i + 1) * 8]
        row = part[:, :128]
        for i in range(1, N // 128):
            row = row + part[:, i * 128 : (i + 1) * 128]
        squares[it] += row
        eb = jnp.concatenate([er.astype(jnp.bfloat16), ei.astype(jnp.bfloat16)], axis=0)
        dims = (((1,), (1,)), ((), ()))
        br = lax.dot_general(eb, whole_r, dims, preferred_element_type=jnp.float32)
        bi = lax.dot_general(eb, whole_i, dims, preferred_element_type=jnp.float32)
        dr = encode(STEP_LENGTH * (qr * er + qi * ei - (br[:R] + bi[R:])))
        di = encode(STEP_LENGTH * (qr * ei - qi * er - (br[R:] - bi[:R])))
        return dr, di

    def publish(it, l):
        u, f = l // RADIX, lax.rem(l, RADIX)
        hr[a, 0, u, f] = hs[a, 0, u, f]
        hr[a, 1, u, f] = hs[a, 1, u, f]

        @pl.when(u == U - 1)
        def _():
            for p in range(halves if it == 0 else 1):
                for j in range(1, A):
                    h_copy(j, f, p).start()

    def product(it, l):
        u, f = l // RADIX, lax.rem(l, RADIX)
        if it == 0:
            re, im = current[0, l], current[1, l]
        else:
            re, im = gr[0, u, f].astype(jnp.float32), gr[1, u, f].astype(jnp.float32)
        dr, di = step_of(it, l, s, re, im)
        for b in range(A):
            hs[b, 0, u, f] = dr[:, b * W : (b + 1) * W]
            hs[b, 1, u, f] = di[:, b * W : (b + 1) * W]
        publish(it, l)

    def lent_product(it, n):
        lend_g(n).wait_recv()
        if it > 0:
            lend_h(n).wait_send()
        dr, di = step_of(
            it, place(F0 * U + n), other, lent_g[0, n].astype(jnp.float32), lent_g[1, n].astype(jnp.float32)
        )
        for b in range(A):
            lent_h[b, 0, n] = dr[:, b * W : (b + 1) * W]
            lent_h[b, 1, n] = di[:, b * W : (b + 1) * W]
        lend_h(n).start()

    def returned(it, n):
        lend_h(n).wait_recv()
        lend_g(n).wait_send()
        publish(it, place(F0 * U + n))

    blocks = half // rows

    def stage_in(it, f, p):
        for j in range(1, A):
            h_copy_in(j, f, p).wait_recv()

        def some(g):
            at = pl.ds(pl.multiple_of(g * rows, rows), rows)
            x = []
            for f2 in range(RADIX):
                b, u = divmod(f2, U)
                l = u * RADIX + f
                re = decode(hr[b, 0, u, f, at, :])
                im = decode(hr[b, 1, u, f, at, :])
                if it == 0:
                    re = re + initial[0, b, l, at, :]
                    im = im + initial[1, b, l, at, :]
                x.append((re * (1.0 / RADIX), im * (1.0 / RADIX)))
            y = eight(x, 1)
            for t in range(RADIX):
                v = rotate(y[t], twiddle[0, f * t], twiddle[1, f * t]) if t else y[t]
                work[0, f, t, at, :] = v[0]
                work[1, f, t, at, :] = v[1]

        loop(p * blocks, p * blocks + blocks, some)

    def stage_time(it, p):
        def some(g):
            at = pl.ds(pl.multiple_of(g * rows, rows), rows)

            def one(t):
                y = eight([(work[0, f, t, at, :], work[1, f, t, at, :]) for f in range(RADIX)], 1)
                if it > 0:
                    y = [(v[0] + traces[0, n, t, at, :], v[1] + traces[1, n, t, at, :]) for n, v in enumerate(y)]
                y = [(shrink(v[0]), shrink(v[1])) for v in y]
                if it < ITERS - 1:
                    for n, v in enumerate(y):
                        traces[0, n, t, at, :] = v[0]
                        traces[1, n, t, at, :] = v[1]
                y = eight(y, -1)
                for f in range(RADIX):
                    v = rotate(y[f], twiddle[0, f * t], -twiddle[1, f * t]) if f else y[f]
                    work[0, f, t, at, :] = v[0]
                    work[1, f, t, at, :] = v[1]

            loop(0, RADIX, one)

        loop(p * blocks, p * blocks + blocks, some)

    def own_out(part, m, p):
        at, pair = strip(p), pl.ds(m * 2, 2)
        return pltpu.make_async_copy(
            gs.at[a, part, :, pair, at], (out_r, out_i)[part].at[:, pair, at, mine], out_sem.at[part, m * halves + p]
        )

    def stage_out(it, f, p):
        def some(g):
            at = pl.ds(pl.multiple_of(g * rows, rows), rows)
            y = eight([(work[0, f, t, at, :], work[1, f, t, at, :]) for t in range(RADIX)], -1)
            for f2 in range(RADIX):
                b, u = divmod(f2, U)
                for part in range(2):
                    v = y[f2][part] * (1.0 / RADIX)
                    gs[b, part, u, f, at, :] = v.astype(jnp.bfloat16) if it == 0 else encode(v)

        loop(p * blocks, p * blocks + blocks, some)

    def give_back(f):
        for p in range(halves):
            stage_out(0, f, p)
        for j in range(1, A):
            g_copy(j, f).start()
        for part in range(2):
            for u in range(U):
                gr[part, u, f, :, mine] = gs[a, part, u, f]

    def give_out(m, p):
        stage_out(1, 2 * m, p)
        stage_out(1, 2 * m + 1, p)
        for j in range(1, A):
            o_copy(0, j, m, p).start()
            o_copy(1, j, m, p).start()
        for part in range(2):
            own_out(part, m, p).start()

    for copy in locals_[:2] + locals_[4:]:
        copy.wait()
    for j in range(1, A):
        for part in range(2):
            initials_in(part, j).wait_recv()

    def last(h):
        @pl.when(keeps(h))
        def _():
            arrive(far, h)
            loop(0, C, lambda chip: across_in(chip, h).wait_recv())

        def slot(i):
            n = h * per * U + i
            if lent:

                @pl.when(is_helper & (n >= F0 * U))
                def _():
                    lent_product(0, n - F0 * U)

                @pl.when(is_end & (n >= F0 * U))
                def _():
                    returned(0, n - F0 * U)

            @pl.when(keeps(h))
            def _():
                product(0, place(n))

            @pl.when((n >= U) & (lax.rem(n, U) == U - 1))
            def _():
                for p in range(halves):
                    stage_in(0, n // U - 1, p)

        loop(0, per * U, slot)

    loop(0, chunks, last)
    for p in range(halves):
        stage_in(0, RADIX - 1, p)
    order = lambda i: lax.rem(F0 + i, RADIX)

    loop(0, halves, lambda p: stage_time(0, p))
    loop(0, RADIX, lambda i: give_back(order(i)))

    def h_sent(f):
        for p in range(halves):
            for j in range(1, A):
                h_copy(j, f, p).wait_send()

    loop(0, RADIX, h_sent)

    def again(i):
        n = lax.rem(F0 * U + i, L)
        l = place(n)

        @pl.when(lax.rem(n, U) == 0)
        def _():
            for j in range(1, A):
                g_copy_in(j, n // U).wait_recv()

        if lent:
            lends = is_end & (n >= F0 * U)

            @pl.when(lends)
            def _():
                lend_g(n - F0 * U).start()

            @pl.when(jnp.logical_not(lends))
            def _():
                product(1, l)

            @pl.when(is_helper & (i >= LAG) & (lax.rem(i, 2) == 0) & (i < 2 * Q + LAG))
            def _():
                lent_product(1, (i - LAG) // 2)

        else:
            product(1, l)

    loop(0, L, again)
    if lent:
        late = (L - LAG + 1) // 2

        @pl.when(is_helper)
        def _():
            if late < Q:
                loop(late, Q, lambda n: lent_product(1, n))

        @pl.when(is_end)
        def _():
            loop(0, Q, lambda n: returned(1, n))


    def rest(f):
        for p in range(1, halves):
            for j in range(1, A):
                h_copy(j, f, p).start()

    loop(0, RADIX, rest)
    by_af[a] = squares[...]

    def af_copy(j):
        return remote(squares, by_af.at[a], m_send.at[j], m_recv.at[j], (ahead(j), s))

    def af_copy_in(j):
        return remote(squares, by_af.at[behind(j)], m_send.at[j], m_recv.at[j], (ahead(j), s))

    for j in range(1, A):
        af_copy(j).start()

    def g_sent(f):
        for j in range(1, A):
            g_copy(j, f).wait_send()

    loop(0, RADIX, g_sent)

    def turn_over(p):
        loop(0, RADIX, lambda i: stage_in(1, order(i + RADIX - F0), p))
        stage_time(1, p)
        loop(0, RADIX // 2, lambda m: give_out(m, p))

    loop(0, halves, turn_over)

    for j in range(1, A):
        af_copy_in(j).wait_recv()
    total = by_af[0]
    for b in range(1, A):
        total = total + by_af[b]
    by_sa[s] = total
    for j in range(1, A):
        af_copy(j).wait_send()
    squares[...] = total

    def sa_copy(j):
        return remote(
            squares, by_sa.at[s], m_send.at[A + j], m_recv.at[A + j], (a, lax.rem(s + j, S))
        )

    def sa_copy_in(j):
        return remote(
            squares, by_sa.at[lax.rem(s + S - j, S)], m_send.at[A + j], m_recv.at[A + j], (a, lax.rem(s + j, S))
        )

    loop(1, S, lambda j: sa_copy(j).start())

    def sent(h):
        @pl.when(goes_up(h))
        def _():
            loop(0, c + 1, lambda chip: up(chip, h).wait_send())

        @pl.when(goes_down(h))
        def _():
            loop(c, C, lambda chip: down(chip, h).wait_send())

        @pl.when(keeps(h))
        def _():
            loop(0, C, lambda chip: across(chip, h).wait_send())

    loop(0, chunks, sent)
    if lent:

        @pl.when(is_helper)
        def _():
            loop(0, Q, lambda n: lend_h(n).wait_send())

    for j in range(1, A):
        for part in range(2):
            initials(part, j).wait_send()
    loop(0, RADIX, h_sent)
    loop(1, S, lambda j: sa_copy_in(j).wait_recv())
    full = by_sa[0]
    for b in range(1, S):
        full = full + by_sa[b]
    for it in range(ITERS):
        mis[it] = jnp.sum(full[it]) * (1.0 / (U * RADIX * A * N * N))
    loop(1, S, lambda j: sa_copy(j).wait_send())

    def finish(m):
        for p in range(halves):
            for j in range(1, A):
                o_both(j, m, p).wait_recv()
                o_both(j, m, p).wait_send()
            for part in range(2):
                own_out(part, m, p).wait()

    loop(0, RADIX // 2, finish)


def on_device(counts, data_real, data_imaginary, wave_real, wave_imaginary, primaries_real, primaries_imaginary):
    A, S = counts
    C = S // 2
    L, R, N = data_real.shape
    W = N // A
    U = L // RADIX
    chunks = RADIX if C <= 8 else 1
    halves = 2 if R % 32 == 0 else 1
    split = lambda v: v.reshape(U, RADIX, R, N)
    kept = RADIX - LENT if C >= 4 and chunks > 1 else RADIX
    Q = max(1, (RADIX - kept) * U)
    turns = 2 * np.pi * np.arange(RADIX * RADIX) / (RADIX * RADIX)
    twiddle = jnp.asarray(np.stack([np.cos(turns), np.sin(turns)]), jnp.float32)
    smem = pl.BlockSpec(memory_space=pltpu.SMEM)
    hbm = pl.BlockSpec(memory_space=pl.ANY)
    vmem = pl.BlockSpec(memory_space=pltpu.VMEM)
    f32, bf16 = jnp.float32, jnp.bfloat16
    dma = pltpu.SemaphoreType.DMA
    coded_r, coded_i, misfit = pl.pallas_call(
        functools.partial(kernel, A, S, chunks, kept),
        in_specs=[smem, smem, smem, hbm, hbm, hbm, hbm],
        out_specs=[hbm, hbm, smem],
        out_shape=[
            pltpu.VMEM((U, RADIX, R, N), bf16),
            pltpu.VMEM((U, RADIX, R, N), bf16),
            jax.ShapeDtypeStruct((ITERS,), f32),
        ],
        scratch_shapes=[
            pltpu.VMEM((U, RADIX, 2, S, R, N), bf16),
            pltpu.VMEM((2, L, R, N), f32),
            pltpu.VMEM((2, A, L, R, W), f32),
            pltpu.VMEM((2, RADIX, RADIX, R, W), f32),
            pltpu.VMEM((2, RADIX, RADIX, R, W), f32),
            pltpu.VMEM((A, 2, U, RADIX, R, W), bf16),
            pltpu.VMEM((A, 2, U, RADIX, R, W), bf16),
            pltpu.VMEM((A, 2, U, RADIX, R, W), bf16),
            pltpu.VMEM((2, U, RADIX, R, N), bf16),
            pltpu.VMEM((ITERS, 8, 128), f32),
            pltpu.VMEM((A, ITERS, 8, 128), f32),
            pltpu.VMEM((S, ITERS, 8, 128), f32),
            pltpu.VMEM((2, Q, R, N), bf16),
            pltpu.VMEM((A, 2, Q, R, W), bf16),
            dma((6,)),
            dma((C, chunks)),
            dma((C, chunks)),
            dma((C, chunks)),
            dma((C, chunks)),
            dma((C, chunks)),
            dma((2, A)),
            dma((2, A)),
            dma((A, RADIX * halves)),
            dma((A, RADIX * halves)),
            dma((A, RADIX)),
            dma((A, RADIX)),
            dma((A, RADIX * halves // 2)),
            dma((A, RADIX * halves // 2)),
            dma((A + S,)),
            dma((A + S,)),
            dma((Q,)),
            dma((Q,)),
            dma((Q,)),
            dma((Q,)),
            dma((2, RADIX * halves // 2)),
        ],
        compiler_params=pltpu.CompilerParams(
            collective_id=0, has_side_effects=True, vmem_limit_bytes=61 * 2**20
        ),
    )(
        wave_real, wave_imaginary, twiddle,
        split(data_real), split(data_imaginary), primaries_real, primaries_imaginary,
    )
    return (decode(coded_r).reshape(L, R, N), decode(coded_i).reshape(L, R, N), misfit)


def solution(mesh):
    split = P("af", "sa", None)
    counts = (mesh.shape["af"], mesh.shape["sa"])
    return jax.shard_map(
        functools.partial(on_device, counts),
        mesh=mesh,
        in_specs=(split, split, P("af"), P("af"), split, split),
        out_specs=(split, split, P()),
        check_vma=False,
    )
```

```python
import functools
import math

import jax
import jax.numpy as jnp
import numpy as np
from jax import lax
from jax.experimental import pallas as pl
from jax.experimental.pallas import tpu as pltpu
from jax.sharding import PartitionSpec as P

ITERS = 2
STEP_LENGTH = 0.02
THRESHOLD = 0.25
RADIX = 8
LENT = 3
LAG = 4
HALF = math.sqrt(0.5)
REACH = 64.0
TINY = 2.0**-126
MESH = pl.DeviceIdType.MESH


def encode(x):
    y = x * (1.0 / REACH)
    return ((y * y) * (y * jnp.abs(y))).astype(jnp.bfloat16)


def decode(code):
    v = code.astype(jnp.float32)
    y = lax.rsqrt(jnp.maximum(jnp.abs(v), TINY))
    return ((v * y) * y) * (lax.rsqrt(y) * REACH)


def add(a, b):
    return (a[0] + b[0], a[1] + b[1])


def sub(a, b):
    return (a[0] - b[0], a[1] - b[1])


def turn(a, sign):
    return (-a[1], a[0]) if sign > 0 else (a[1], -a[0])


def rotate(a, c, s):
    return (a[0] * c - a[1] * s, a[0] * s + a[1] * c)


def four(a, b, c, d, sign):
    s0, s1, s2, s3 = add(a, c), sub(a, c), add(b, d), turn(sub(b, d), sign)
    return add(s0, s2), add(s1, s3), sub(s0, s2), sub(s1, s3)


def eight(x, sign):
    even = four(x[0], x[2], x[4], x[6], sign)
    odd = four(x[1], x[3], x[5], x[7], sign)
    o1 = add(odd[1], turn(odd[1], sign))
    o3 = sub(turn(odd[3], sign), odd[3])
    odd = (odd[0], (o1[0] * HALF, o1[1] * HALF), turn(odd[2], sign), (o3[0] * HALF, o3[1] * HALF))
    return [add(even[k], odd[k]) for k in range(4)] + [sub(even[k], odd[k]) for k in range(4)]


def shrink(v):
    return v - jnp.clip(v, -THRESHOLD, THRESHOLD)


def loop(start, stop, body):
    def step(i, _):
        body(i)
        return 0

    lax.fori_loop(start, stop, step, 0)


def kernel(
    A, S, chunks, F0, wr, wi, twiddle, data_r, data_i, prim_r, prim_i, out_r, out_i, mis,
    whole, current, initial, work, traces, hs, hr, gs, gr, squares, by_af, by_sa, lent_g, lent_h,
    local_sem, up_sem, down_sem, ring_sem, pair_send, pair_recv,
    init_send, init_recv, h_send, h_recv, g_send, g_recv, o_send, o_recv, m_send, m_recv,
    lg_send, lg_recv, lh_send, lh_recv, d_send, d_recv, out_sem,
):
    C = S // 2
    L, R, N = prim_r.shape
    U = L // RADIX
    W = N // A
    per = RADIX // chunks
    halves = 2 if R % 32 == 0 else 1
    half = R // halves
    rows = 16 if R % 16 == 0 else 8
    a = lax.axis_index("af")
    s = lax.axis_index("sa")
    c = s // 2
    k = s % 2
    partner = c * 2 + 1 - k
    kept = F0 // per
    lent = chunks - kept
    Q = L - F0 * U
    if lent:
        is_end = (c == 0) | (c == C - 1)
        is_helper = (c == 1) | (c == C - 2)
        other = jnp.where((c == 0) | (c == C - 2), s + 2, s - 2)
        lender = is_end | is_helper

    def goes_up(h):
        go = c + 1 < C
        return go & ((h < kept) | (c + 2 < C)) if lent else go

    def goes_down(h):
        go = c > 0
        return go & ((h < kept) | (c > 1)) if lent else go

    def keeps(h):
        return (h < kept) | jnp.logical_not(is_end) if lent else h >= 0

    mine = pl.ds(pl.multiple_of(a * W, W), W)

    def place(n):
        return lax.rem(n, U) * RADIX + n // U

    def cols(b):
        return pl.ds(pl.multiple_of(b * W, W), W)

    def ahead(j):
        return lax.rem(a + j, A)

    def behind(j):
        return lax.rem(a + A - j, A)

    barrier = pltpu.get_barrier_semaphore()
    for j in range(1, A):
        pl.semaphore_signal(barrier, inc=1, device_id=(ahead(j), s), device_id_type=MESH)
    loop(
        1, S,
        lambda j: pl.semaphore_signal(barrier, inc=1, device_id=(a, lax.rem(s + j, S)), device_id_type=MESH),
    )

    greeted = A - 1 + S - 1
    if lent:

        @pl.when(lender)
        def _():
            for j in range(1, A):
                pl.semaphore_signal(barrier, inc=1, device_id=(ahead(j), other), device_id_type=MESH)

        greeted = greeted + jnp.where(lender, A - 1, 0)

    locals_ = [
        pltpu.make_async_copy(data_r, whole.at[:, :, 0, s], local_sem.at[0]),
        pltpu.make_async_copy(data_i, whole.at[:, :, 1, s], local_sem.at[1]),
        pltpu.make_async_copy(prim_r, current.at[0], local_sem.at[2]),
        pltpu.make_async_copy(prim_i, current.at[1], local_sem.at[3]),
        pltpu.make_async_copy(prim_r.at[:, :, mine], initial.at[0, a], local_sem.at[4]),
        pltpu.make_async_copy(prim_i.at[:, :, mine], initial.at[1, a], local_sem.at[5]),
    ]
    for copy in locals_:
        copy.start()
    squares[...] = jnp.zeros_like(squares)
    pl.semaphore_wait(barrier, greeted)

    def shard(chip, core, h):
        return whole.at[:, pl.ds(h * per, per), :, chip * 2 + core]

    def remote(src, dst, send, recv, device):
        return pltpu.make_async_remote_copy(
            src_ref=src, dst_ref=dst, send_sem=send, recv_sem=recv, device_id=device, device_id_type=MESH
        )

    def own(part, h):
        return (data_r, data_i)[part].at[:, pl.ds(h * per, per)]

    def up(chip, h):
        ref = shard(chip, k, h)
        return remote(ref, ref, up_sem.at[chip, h], ring_sem.at[chip, h], (a, lax.rem(s + 2, S)))

    def down(chip, h):
        ref = shard(chip, k, h)
        return remote(ref, ref, down_sem.at[chip, h], ring_sem.at[chip, h], (a, lax.rem(s + S - 2, S)))

    def across(chip, h):
        ref = shard(chip, k, h)
        return remote(ref, ref, pair_send.at[chip, h], pair_recv.at[chip, h], (a, partner))

    def own_up(part, h):
        return remote(
            own(part, h), shard(c, k, h).at[:, :, part], up_sem.at[c, h], ring_sem.at[c, h], (a, lax.rem(s + 2, S))
        )

    def own_down(part, h):
        return remote(
            own(part, h), shard(c, k, h).at[:, :, part], down_sem.at[c, h], ring_sem.at[c, h], (a, lax.rem(s + S - 2, S))
        )

    def own_across(part, h):
        return remote(
            own(part, h), shard(c, k, h).at[:, :, part], pair_send.at[c, h], pair_recv.at[c, h], (a, partner)
        )

    def across_in(chip, h):
        ref = shard(chip, 1 - k, h)
        return remote(ref, ref, pair_send.at[chip, h], pair_recv.at[chip, h], (a, partner))

    def initials(part, j):
        src = (prim_r, prim_i)[part]
        return remote(
            src.at[:, :, cols(ahead(j))], initial.at[part, a],
            init_send.at[part, j], init_recv.at[part, j], (ahead(j), s),
        )

    def initials_in(part, j):
        src = (prim_r, prim_i)[part]
        return remote(
            src.at[:, :, mine], initial.at[part, behind(j)],
            init_send.at[part, j], init_recv.at[part, j], (ahead(j), s),
        )

    def first(h):
        @pl.when(goes_up(h))
        def _():
            own_up(0, h).start()
            own_up(1, h).start()

        @pl.when(goes_down(h))
        def _():
            own_down(0, h).start()
            own_down(1, h).start()

        @pl.when(keeps(h))
        def _():
            own_across(0, h).start()
            own_across(1, h).start()

    loop(0, chunks, first)

    def lend_g(n):
        return remote(gr.at[:, lax.rem(n, U), F0 + n // U], lent_g.at[:, n], lg_send.at[n], lg_recv.at[n], (a, other))

    def lend_first(n):
        return remote(lent_g.at[:, n], lent_g.at[:, n], lg_send.at[n], lg_recv.at[n], (a, other))

    def lend_h(n):
        return remote(lent_h.at[:, :, n], hs.at[:, :, lax.rem(n, U), F0 + n // U], lh_send.at[n], lh_recv.at[n], (a, other))

    for j in range(1, A):
        for part in range(2):
            initials(part, j).start()
    for copy in locals_[2:4]:
        copy.wait()
    if lent:

        @pl.when(is_end)
        def _():
            def lend(n):
                at = place(F0 * U + n)
                for part in range(2):
                    lent_g[part, n] = current[part, at].astype(jnp.bfloat16)
                lend_first(n).start()

            loop(0, Q, lend)


    def arrive(d, h):
        @pl.when(c >= d)
        def _():
            src = c - d
            up(src, h).wait_recv()
            across(src, h).start()

            @pl.when(goes_up(h))
            def _():
                up(src, h).start()

        @pl.when(c + d < C)
        def _():
            src = c + d
            down(src, h).wait_recv()
            across(src, h).start()

            @pl.when(goes_down(h))
            def _():
                down(src, h).start()

    far = jnp.maximum(c, C - 1 - c)

    def pass_on(h, d):
        @pl.when(keeps(h))
        def _():
            arrive(d, h)

    loop(1, far, lambda d: loop(0, chunks, lambda h: pass_on(h, d)))

    def strip(p):
        return pl.ds(pl.multiple_of(p * half, half), half)

    def h_copy(j, f, p):
        to, q, at = ahead(j), f * halves + p, strip(p)
        return remote(hs.at[to, :, :, f, at], hr.at[a, :, :, f, at], h_send.at[j, q], h_recv.at[j, q], (to, s))

    def h_copy_in(j, f, p):
        q, at = f * halves + p, strip(p)
        return remote(
            hs.at[a, :, :, f, at], hr.at[behind(j), :, :, f, at], h_send.at[j, q], h_recv.at[j, q], (ahead(j), s)
        )

    def g_copy(j, f):
        to = ahead(j)
        return remote(gs.at[to, :, :, f], gr.at[:, :, f, :, mine], g_send.at[j, f], g_recv.at[j, f], (to, s))

    def g_copy_in(j, f):
        return remote(
            gs.at[a, :, :, f], gr.at[:, :, f, :, cols(behind(j))], g_send.at[j, f], g_recv.at[j, f], (ahead(j), s)
        )

    def o_copy(part, j, m, p):
        to, q, at, pair = ahead(j), m * halves + p, strip(p), pl.ds(m * 2, 2)
        return remote(
            gs.at[to, part, :, pair, at], (out_r, out_i)[part].at[:, pair, at, mine],
            o_send.at[j, q], o_recv.at[j, q], (to, s),
        )

    def o_both(j, m, p):
        q, at, pair = m * halves + p, strip(p), pl.ds(m * 2, 2)
        return remote(
            gs.at[a, :, :, pair, at], gr.at[:, :, pair, at, cols(behind(j))],
            o_send.at[j, q], o_recv.at[j, q], (ahead(j), s),
        )

    def step_of(it, l, at, re, im):
        u, f = l // RADIX, lax.rem(l, RADIX)
        qr = wr[l]
        qi = wi[l]
        whole_r = whole[u, f, 0].reshape(N, N)
        whole_i = whole[u, f, 1].reshape(N, N)
        left = jnp.concatenate([re.astype(jnp.bfloat16), im.astype(jnp.bfloat16)], axis=0)
        pr = jnp.dot(left, whole_r, preferred_element_type=jnp.float32)
        pi = jnp.dot(left, whole_i, preferred_element_type=jnp.float32)
        er = whole[u, f, 0, at].astype(jnp.float32) + (pr[:R] - pi[R:]) - (qr * re - qi * im)
        ei = whole[u, f, 1, at].astype(jnp.float32) + (pi[:R] + pr[R:]) - (qr * im + qi * re)
        sq = er * er + ei * ei
        part = sq[:8]
        for i in range(1, R // 8):
            part = part + sq[i * 8 : (i + 1) * 8]
        row = part[:, :128]
        for i in range(1, N // 128):
            row = row + part[:, i * 128 : (i + 1) * 128]
        squares[it] += row
        eb = jnp.concatenate([er.astype(jnp.bfloat16), ei.astype(jnp.bfloat16)], axis=0)
        dims = (((1,), (1,)), ((), ()))
        br = lax.dot_general(eb, whole_r, dims, preferred_element_type=jnp.float32)
        bi = lax.dot_general(eb, whole_i, dims, preferred_element_type=jnp.float32)
        dr = encode(STEP_LENGTH * (qr * er + qi * ei - (br[:R] + bi[R:])))
        di = encode(STEP_LENGTH * (qr * ei - qi * er - (br[R:] - bi[:R])))
        return dr, di

    def direct(j, n):
        to = ahead(j)
        return remote(
            lent_h.at[to, :, n], hr.at[a, :, lax.rem(n, U), F0 + n // U], d_send.at[j, n], d_recv.at[j, n], (to, other)
        )

    def direct_in(j, n):
        return remote(
            lent_h.at[a, :, n], hr.at[behind(j), :, lax.rem(n, U), F0 + n // U],
            d_send.at[j, n], d_recv.at[j, n], (ahead(j), other),
        )

    def publish(it, l):
        u, f = l // RADIX, lax.rem(l, RADIX)
        hr[a, 0, u, f] = hs[a, 0, u, f]
        hr[a, 1, u, f] = hs[a, 1, u, f]

        @pl.when(u == U - 1)
        def _():
            for p in range(halves if it == 0 else 1):
                for j in range(1, A):
                    h_copy(j, f, p).start()

    def product(it, l):
        u, f = l // RADIX, lax.rem(l, RADIX)
        if it == 0:
            re, im = current[0, l], current[1, l]
        else:
            re, im = gr[0, u, f].astype(jnp.float32), gr[1, u, f].astype(jnp.float32)
        dr, di = step_of(it, l, s, re, im)
        for b in range(A):
            hs[b, 0, u, f] = dr[:, b * W : (b + 1) * W]
            hs[b, 1, u, f] = di[:, b * W : (b + 1) * W]
        publish(it, l)

    def lent_product(it, n):
        lend_g(n).wait_recv()
        if it > 0:
            for j in range(A):
                direct(j, n).wait_send()
        dr, di = step_of(
            it, place(F0 * U + n), other, lent_g[0, n].astype(jnp.float32), lent_g[1, n].astype(jnp.float32)
        )
        for b in range(A):
            lent_h[b, 0, n] = dr[:, b * W : (b + 1) * W]
            lent_h[b, 1, n] = di[:, b * W : (b + 1) * W]
        if it > 0:
            lend_h(n).start()
        else:
            for j in range(A):
                direct(j, n).start()

    def returned(it, n):
        lend_h(n).wait_recv()
        lend_g(n).wait_send()
        publish(it, place(F0 * U + n))

    blocks = half // rows

    def stage_in(it, f, p):
        if lent and it == 0:
            by_lender = is_end & (f >= F0)

            @pl.when(by_lender & (p == 0))
            def _():
                for u in range(U):
                    n = (f - F0) * U + u
                    lend_first(n).wait_send()
                    for j in range(A):
                        direct_in(j, n).wait_recv()

            @pl.when(jnp.logical_not(by_lender))
            def _():
                for j in range(1, A):
                    h_copy_in(j, f, p).wait_recv()

        else:
            for j in range(1, A):
                h_copy_in(j, f, p).wait_recv()

        def some(g):
            at = pl.ds(pl.multiple_of(g * rows, rows), rows)
            x = []
            for f2 in range(RADIX):
                b, u = divmod(f2, U)
                l = u * RADIX + f
                re = decode(hr[b, 0, u, f, at, :])
                im = decode(hr[b, 1, u, f, at, :])
                if it == 0:
                    re = re + initial[0, b, l, at, :]
                    im = im + initial[1, b, l, at, :]
                x.append((re * (1.0 / RADIX), im * (1.0 / RADIX)))
            y = eight(x, 1)
            for t in range(RADIX):
                v = rotate(y[t], twiddle[0, f * t], twiddle[1, f * t]) if t else y[t]
                work[0, f, t, at, :] = v[0]
                work[1, f, t, at, :] = v[1]

        loop(p * blocks, p * blocks + blocks, some)

    def stage_time(it, p):
        def some(g):
            at = pl.ds(pl.multiple_of(g * rows, rows), rows)

            def one(t):
                y = eight([(work[0, f, t, at, :], work[1, f, t, at, :]) for f in range(RADIX)], 1)
                if it > 0:
                    y = [(v[0] + traces[0, n, t, at, :], v[1] + traces[1, n, t, at, :]) for n, v in enumerate(y)]
                y = [(shrink(v[0]), shrink(v[1])) for v in y]
                if it < ITERS - 1:
                    for n, v in enumerate(y):
                        traces[0, n, t, at, :] = v[0]
                        traces[1, n, t, at, :] = v[1]
                y = eight(y, -1)
                for f in range(RADIX):
                    v = rotate(y[f], twiddle[0, f * t], -twiddle[1, f * t]) if f else y[f]
                    work[0, f, t, at, :] = v[0]
                    work[1, f, t, at, :] = v[1]

            loop(0, RADIX, one)

        loop(p * blocks, p * blocks + blocks, some)

    def own_out(part, m, p):
        at, pair = strip(p), pl.ds(m * 2, 2)
        return pltpu.make_async_copy(
            gs.at[a, part, :, pair, at], (out_r, out_i)[part].at[:, pair, at, mine], out_sem.at[part, m * halves + p]
        )

    def stage_out(it, f, p):
        def some(g):
            at = pl.ds(pl.multiple_of(g * rows, rows), rows)
            y = eight([(work[0, f, t, at, :], work[1, f, t, at, :]) for t in range(RADIX)], -1)
            for f2 in range(RADIX):
                b, u = divmod(f2, U)
                for part in range(2):
                    v = y[f2][part] * (1.0 / RADIX)
                    gs[b, part, u, f, at, :] = v.astype(jnp.bfloat16) if it == 0 else encode(v)

        loop(p * blocks, p * blocks + blocks, some)

    def give_back(f):
        for p in range(halves):
            stage_out(0, f, p)
        for j in range(1, A):
            g_copy(j, f).start()
        for part in range(2):
            for u in range(U):
                gr[part, u, f, :, mine] = gs[a, part, u, f]

    def give_out(m, p):
        stage_out(1, 2 * m, p)
        stage_out(1, 2 * m + 1, p)
        for j in range(1, A):
            o_copy(0, j, m, p).start()
            o_copy(1, j, m, p).start()
        for part in range(2):
            own_out(part, m, p).start()

    for copy in locals_[:2] + locals_[4:]:
        copy.wait()
    for j in range(1, A):
        for part in range(2):
            initials_in(part, j).wait_recv()

    def last(h):
        @pl.when(keeps(h))
        def _():
            arrive(far, h)
            loop(0, C, lambda chip: across_in(chip, h).wait_recv())

        def slot(i):
            n = h * per * U + i
            if lent:

                @pl.when(is_helper & (n >= F0 * U))
                def _():
                    lent_product(0, n - F0 * U)

            @pl.when(keeps(h))
            def _():
                product(0, place(n))

            @pl.when((n >= U) & (lax.rem(n, U) == U - 1))
            def _():
                for p in range(halves):
                    stage_in(0, n // U - 1, p)

        loop(0, per * U, slot)

    loop(0, chunks, last)
    for p in range(halves):
        stage_in(0, RADIX - 1, p)
    order = lambda i: lax.rem(F0 + i, RADIX)

    loop(0, halves, lambda p: stage_time(0, p))
    loop(0, RADIX, lambda i: give_back(order(i)))

    def h_sent(f):
        for p in range(halves):
            for j in range(1, A):
                h_copy(j, f, p).wait_send()

    loop(0, jnp.where(is_end, F0, RADIX) if lent else RADIX, h_sent)

    def again(i):
        n = lax.rem(F0 * U + i, L)
        l = place(n)

        @pl.when(lax.rem(n, U) == 0)
        def _():
            for j in range(1, A):
                g_copy_in(j, n // U).wait_recv()

        if lent:
            lends = is_end & (n >= F0 * U)

            @pl.when(lends)
            def _():
                lend_g(n - F0 * U).start()

            @pl.when(jnp.logical_not(lends))
            def _():
                product(1, l)

            @pl.when(is_helper & (i >= LAG) & (lax.rem(i, 2) == 0) & (i < 2 * Q + LAG))
            def _():
                lent_product(1, (i - LAG) // 2)

        else:
            product(1, l)

    loop(0, L, again)
    if lent:
        late = (L - LAG + 1) // 2

        @pl.when(is_helper)
        def _():
            if late < Q:
                loop(late, Q, lambda n: lent_product(1, n))

        @pl.when(is_end)
        def _():
            loop(0, Q, lambda n: returned(1, n))


    def rest(f):
        for p in range(1, halves):
            for j in range(1, A):
                h_copy(j, f, p).start()

    loop(0, RADIX, rest)
    by_af[a] = squares[...]

    def af_copy(j):
        return remote(squares, by_af.at[a], m_send.at[j], m_recv.at[j], (ahead(j), s))

    def af_copy_in(j):
        return remote(squares, by_af.at[behind(j)], m_send.at[j], m_recv.at[j], (ahead(j), s))

    for j in range(1, A):
        af_copy(j).start()

    def g_sent(f):
        for j in range(1, A):
            g_copy(j, f).wait_send()

    loop(0, RADIX, g_sent)

    def turn_over(p):
        loop(0, RADIX, lambda i: stage_in(1, order(i + RADIX - F0), p))
        stage_time(1, p)
        loop(0, RADIX // 2, lambda m: give_out(m, p))

    loop(0, halves, turn_over)

    for j in range(1, A):
        af_copy_in(j).wait_recv()
    total = by_af[0]
    for b in range(1, A):
        total = total + by_af[b]
    by_sa[s] = total
    for j in range(1, A):
        af_copy(j).wait_send()
    squares[...] = total

    def sa_copy(j):
        return remote(
            squares, by_sa.at[s], m_send.at[A + j], m_recv.at[A + j], (a, lax.rem(s + j, S))
        )

    def sa_copy_in(j):
        return remote(
            squares, by_sa.at[lax.rem(s + S - j, S)], m_send.at[A + j], m_recv.at[A + j], (a, lax.rem(s + j, S))
        )

    loop(1, S, lambda j: sa_copy(j).start())

    def sent(h):
        @pl.when(goes_up(h))
        def _():
            loop(0, c + 1, lambda chip: up(chip, h).wait_send())

        @pl.when(goes_down(h))
        def _():
            loop(c, C, lambda chip: down(chip, h).wait_send())

        @pl.when(keeps(h))
        def _():
            loop(0, C, lambda chip: across(chip, h).wait_send())

    loop(0, chunks, sent)
    if lent:

        @pl.when(is_helper)
        def _():
            loop(0, Q, lambda n: lend_h(n).wait_send())

    for j in range(1, A):
        for part in range(2):
            initials(part, j).wait_send()
    loop(0, RADIX, h_sent)
    loop(1, S, lambda j: sa_copy_in(j).wait_recv())
    full = by_sa[0]
    for b in range(1, S):
        full = full + by_sa[b]
    for it in range(ITERS):
        mis[it] = jnp.sum(full[it]) * (1.0 / (U * RADIX * A * N * N))
    loop(1, S, lambda j: sa_copy(j).wait_send())

    def finish(m):
        for p in range(halves):
            for j in range(1, A):
                o_both(j, m, p).wait_recv()
                o_both(j, m, p).wait_send()
            for part in range(2):
                own_out(part, m, p).wait()

    loop(0, RADIX // 2, finish)


def on_device(counts, data_real, data_imaginary, wave_real, wave_imaginary, primaries_real, primaries_imaginary):
    A, S = counts
    C = S // 2
    L, R, N = data_real.shape
    W = N // A
    U = L // RADIX
    chunks = RADIX if C <= 8 else 1
    halves = 2 if R % 32 == 0 else 1
    split = lambda v: v.reshape(U, RADIX, R, N)
    kept = RADIX - LENT if C >= 4 and chunks > 1 else RADIX
    Q = max(1, (RADIX - kept) * U)
    turns = 2 * np.pi * np.arange(RADIX * RADIX) / (RADIX * RADIX)
    twiddle = jnp.asarray(np.stack([np.cos(turns), np.sin(turns)]), jnp.float32)
    smem = pl.BlockSpec(memory_space=pltpu.SMEM)
    hbm = pl.BlockSpec(memory_space=pl.ANY)
    vmem = pl.BlockSpec(memory_space=pltpu.VMEM)
    f32, bf16 = jnp.float32, jnp.bfloat16
    dma = pltpu.SemaphoreType.DMA
    coded_r, coded_i, misfit = pl.pallas_call(
        functools.partial(kernel, A, S, chunks, kept),
        in_specs=[smem, smem, smem, hbm, hbm, hbm, hbm],
        out_specs=[hbm, hbm, smem],
        out_shape=[
            pltpu.VMEM((U, RADIX, R, N), bf16),
            pltpu.VMEM((U, RADIX, R, N), bf16),
            jax.ShapeDtypeStruct((ITERS,), f32),
        ],
        scratch_shapes=[
            pltpu.VMEM((U, RADIX, 2, S, R, N), bf16),
            pltpu.VMEM((2, L, R, N), f32),
            pltpu.VMEM((2, A, L, R, W), f32),
            pltpu.VMEM((2, RADIX, RADIX, R, W), f32),
            pltpu.VMEM((2, RADIX, RADIX, R, W), f32),
            pltpu.VMEM((A, 2, U, RADIX, R, W), bf16),
            pltpu.VMEM((A, 2, U, RADIX, R, W), bf16),
            pltpu.VMEM((A, 2, U, RADIX, R, W), bf16),
            pltpu.VMEM((2, U, RADIX, R, N), bf16),
            pltpu.VMEM((ITERS, 8, 128), f32),
            pltpu.VMEM((A, ITERS, 8, 128), f32),
            pltpu.VMEM((S, ITERS, 8, 128), f32),
            pltpu.VMEM((2, Q, R, N), bf16),
            pltpu.VMEM((A, 2, Q, R, W), bf16),
            dma((6,)),
            dma((C, chunks)),
            dma((C, chunks)),
            dma((C, chunks)),
            dma((C, chunks)),
            dma((C, chunks)),
            dma((2, A)),
            dma((2, A)),
            dma((A, RADIX * halves)),
            dma((A, RADIX * halves)),
            dma((A, RADIX)),
            dma((A, RADIX)),
            dma((A, RADIX * halves // 2)),
            dma((A, RADIX * halves // 2)),
            dma((A + S,)),
            dma((A + S,)),
            dma((Q,)),
            dma((Q,)),
            dma((Q,)),
            dma((Q,)),
            dma((A, Q)),
            dma((A, Q)),
            dma((2, RADIX * halves // 2)),
        ],
        compiler_params=pltpu.CompilerParams(
            collective_id=0, has_side_effects=True, vmem_limit_bytes=61 * 2**20
        ),
    )(
        wave_real, wave_imaginary, twiddle,
        split(data_real), split(data_imaginary), primaries_real, primaries_imaginary,
    )
    return (decode(coded_r).reshape(L, R, N), decode(coded_i).reshape(L, R, N), misfit)


def solution(mesh):
    split = P("af", "sa", None)
    counts = (mesh.shape["af"], mesh.shape["sa"])
    return jax.shard_map(
        functools.partial(on_device, counts),
        mesh=mesh,
        in_specs=(split, split, P("af"), P("af"), split, split),
        out_specs=(split, split, P()),
        check_vma=False,
    )
```
